512 devices in a mesh: rep: 4 (over y), fsdp: 128 (over x, z, core).
Axes of the slice: x: 4, y: 4, z: 16, core: 2. Of those that a mesh axis runs over, the one named last changes fastest.
Arguments:
- momentum: float32 [4, 18432, 2304], P('rep', 'fsdp'), may hold values from -60 to 60
- gradient: bfloat16 [4, 18432, 2304], P('rep', 'fsdp'), may hold values from -30 to 30
- right_factor: float32 [2304, 256], P('fsdp'), may hold values from -0.125 to 0.125
Outputs:
- new_momentum: float32 [4, 18432, 2304], P('rep', 'fsdp')
- update: bfloat16 [18432, 2304], P('fsdp')
- new_factor: float32 [2304, 256], P('fsdp')
The draws below stay inside these ranges and needn't reach their ends.
All inputs are finite; a program needn't handle non-finite values.
Results may differ from the reference program's by a relative error of at most 0.001.
Values sent between devices are 32-bit elements; how exact they have to be, the bound alone decides.
A program may use at most 64 MiB of HBM per device.

```python
import math
import jax
import jax.numpy as jnp
from jax import lax

ROWS = 18432
COLS = 2304
RANK = 256
REPLICAS = 4


def column_scales(key):
    scale_key = jax.random.fold_in(key, 11)
    rising = jnp.exp(jnp.log(10.0) * jnp.arange(COLS, dtype=jnp.float32) / COLS)
    jitter = jnp.exp(jax.random.uniform(scale_key, (COLS,), jnp.float32, -0.4, 0.4))
    return 0.3 * rising * jitter


def clipped_normal(key, shape):
    return jnp.clip(jax.random.normal(key, shape, jnp.float32), -6.0, 6.0)


def draw_momentum(key, part):
    scales = column_scales(key)
    values = 2.0 * clipped_normal(jax.random.fold_in(key, 1), (REPLICAS, ROWS, COLS)) * scales
    return values.astype(jnp.float32)


def draw_gradient(key, part):
    scales = column_scales(key)
    values = clipped_normal(jax.random.fold_in(key, 2), (REPLICAS, ROWS, COLS)) * scales
    return values.astype(jnp.bfloat16)


def level_of(stream_key, shape, shards, smallest, top_value):
    gain, own = 1.0, jax.random.fold_in(stream_key, 6)
    for dim, shards_of in shards:
        draws = jnp.exp(jax.random.uniform(jax.random.fold_in(own, dim), (shards_of,), jnp.float32, smallest / len(shards), top_value / len(shards)))
        gain = gain * jnp.repeat(draws, shape[dim] // shards_of).reshape([-1 if axis == dim else 1 for axis in range(len(shape))])
    return gain


def bell_draw(stream_key, dims, width, reach, cuts=(), held_as=jnp.bfloat16):
    entries = jax.random.normal(stream_key, dims, jnp.float32) * width
    if len(cuts) > 0:
        entries = level_of(stream_key, dims, cuts, -0.22, 0.18) * entries
    return jnp.clip(entries, min=-reach, max=reach).astype(held_as)


def setup_inputs(seed: int = 0) -> dict:
    key_of = jax.random.split(jax.random.key(seed), 4)
    momentum = draw_momentum(jax.random.fold_in(key_of[3], 71), 0)
    gradient = draw_gradient(jax.random.fold_in(key_of[3], 71), 0)
    right_factor = bell_draw(key_of[2], (COLS, RANK), COLS ** -0.5, 0.125, ((0, 128),), jnp.float32)
    return {"momentum": momentum, "gradient": gradient, "right_factor": right_factor}


epsilon = 1e-06
decay_rate = 0.95
highest = lax.Precision.HIGHEST

def reference(momentum, gradient, right_factor):
    buffer = momentum + gradient.astype(jnp.float32)
    projected = jnp.einsum('irc,ck->rk', buffer, right_factor, precision=highest)
    gram_matrix = jnp.dot(projected.T.astype(jnp.float32), projected.astype(jnp.float32), precision=highest, preferred_element_type=jnp.float32)
    lower_factor = jnp.linalg.cholesky(gram_matrix)
    orthonormal = jax.scipy.linalg.solve_triangular(lower_factor, projected.T, lower=True).T
    factor = jnp.einsum('irc,rk->ck', buffer, orthonormal, precision=highest) / REPLICAS
    col_norms = jnp.sqrt(lax.optimization_barrier(jnp.sum(factor * factor, axis=0)) + epsilon)
    new_factor = factor / col_norms
    correction = jnp.dot(orthonormal.astype(jnp.float32), factor.T.astype(jnp.float32), precision=highest, preferred_element_type=jnp.float32)
    new_momentum = buffer - (1.0 - decay_rate) * correction[None]
    scaled = math.sqrt(ROWS * COLS / RANK) * jnp.dot(orthonormal.astype(jnp.float32), new_factor.T.astype(jnp.float32), precision=highest, preferred_element_type=jnp.float32)
    return (new_momentum, scaled.astype(jnp.bfloat16), new_factor)
```

```python
import math

import jax
import jax.numpy as jnp
from jax import lax
from jax.experimental import pallas as pl
from jax.experimental.pallas import tpu as pltpu
from jax.sharding import Mesh
from jax.sharding import PartitionSpec as P

ROWS = 18432
COLS = 2304
RANK = 256
REPLICAS = 4
FSDP = ("fx", "fz", "fc")

NX, NZ = 4, 16
SHARD = ROWS // 128
BLOCK = COLS // 4
OWN = COLS // 128
PIECE = 80
FACTOR_ROWS = 72
TILES = PIECE // 8

epsilon = 1e-06
decay_rate = 0.95
highest = lax.Precision.HIGHEST
MESH = pl.DeviceIdType.MESH
VMEM = pltpu.VMEM
f32 = jnp.float32


def copy_to(src, dst, send, recv, device):
    return pltpu.make_async_remote_copy(
        src_ref=src,
        dst_ref=dst,
        send_sem=send,
        recv_sem=recv,
        device_id=device,
        device_id_type=MESH,
    )


def gather_ring(block, me, right, left, send, recv):
    before, after, across = (me + 3) % 4, (me + 1) % 4, (me + 2) % 4

    def hop(q, h, device, i):
        return copy_to(block(q, h), block(q, h), send.at[i], recv.at[i], device)

    first = [hop(me, 0, right, 0), hop(me, 1, left, 1), hop(me, 1, right, 2), hop(me, 0, left, 3)]
    for copy in first:
        copy.start()
    first[0].wait_recv()
    onward = hop(before, 0, right, 4)
    onward.start()
    first[1].wait_recv()
    backward = hop(after, 1, left, 5)
    backward.start()
    first[2].wait_recv()
    first[3].wait_recv()
    onward.wait_recv()
    backward.wait_recv()
    for copy in first + [onward, backward]:
        copy.wait_send()


def exchange_kernel(
    m_hbm, g_hbm, r_hbm, p_out, mall,
    mv, gv, bs, raw, comb, cin, inn, s_c, rall, rc, pall, gram, mloc, crecv, mx, xrecv, mz, zrecv, fin,
    load, s_send, s_recv, rx_send, rx_recv, rz_send, rz_recv, rc_send, rc_recv, p_send, p_recv,
    c_send, c_recv, x_send, x_recv, z_send, z_recv, f_send, f_recv, a_send, a_recv, b_send, b_recv,
    d_send, d_recv,
):
    y, x, z, c = (lax.axis_index(name) for name in ("rep",) + FSDP)

    def at_y(q):
        return (q, x, z, c)

    def at_x(q):
        return (y, q, z, c)

    def at_z(q):
        return (y, x, q, c)

    partner = (y, x, z, 1 - c)
    peers = [at_y((y + d) % 4) for d in range(1, 4)]
    peers += [at_x((x + d) % 4) for d in range(1, 4)]
    peers += [at_z((z + d) % NZ) for d in range(1, NZ)]
    peers += [partner]
    barrier = pltpu.get_barrier_semaphore()
    for peer in peers:
        pl.semaphore_signal(barrier, inc=1, device_id=peer, device_id_type=MESH)

    source = x == y
    load_m = pltpu.make_async_copy(m_hbm.at[0], mv, load.at[0])
    load_g = pltpu.make_async_copy(g_hbm.at[0], gv, load.at[1])
    load_r = pltpu.make_async_copy(r_hbm, rall.at[z, c], load.at[2])

    @pl.when(source)
    def _():
        load_r.start()

    load_m.start()
    load_g.start()

    @pl.when(source)
    def _():
        load_r.wait()

    pl.semaphore_wait(barrier, len(peers))

    to_x = [
        copy_to(rall.at[z, c], rall.at[z, c], rx_send.at[d - 1], rx_recv.at[0], at_x((x + d) % 4))
        for d in range(1, 4)
    ]

    @pl.when(source)
    def _():
        for copy in to_x:
            copy.start()

    load_m.wait()
    load_g.wait()
    for q in range(4):
        columns = slice(q * BLOCK, (q + 1) * BLOCK)
        bs[q] = mv[:, columns] + gv[:, columns].astype(f32)

    half = SHARD // 2
    up, down = at_y((y + 1) % 4), at_y((y + 3) % 4)
    after, before, across = (y + 1) % 4, (y + 3) % 4, (y + 2) % 4
    low, high = pl.ds(0, half), pl.ds(half, half)
    sums = [
        copy_to(bs.at[across, low], raw.at[0], s_send.at[0], s_recv.at[0], up),
        copy_to(bs.at[across, high], raw.at[1], s_send.at[1], s_recv.at[1], down),
        copy_to(bs.at[after, high], inn.at[1], s_send.at[2], s_recv.at[2], up),
        copy_to(bs.at[before, low], inn.at[0], s_send.at[3], s_recv.at[3], down),
    ]
    for copy in sums:
        copy.start()

    @pl.when(jnp.logical_not(source))
    def _():
        to_x[0].wait_recv()

    order = sorted(range(1, NZ), key=lambda d: abs(d - NZ // 2))
    to_z = [
        copy_to(rall.at[z, c], rall.at[z, c], rz_send.at[d - 1], rz_recv.at[d - 1], at_z((z + d) % NZ))
        for d in order
    ]
    for copy in to_z:
        copy.start()

    sums[0].wait_recv()
    comb[0] = raw[0] + bs[after, :half]
    sums.append(copy_to(comb.at[0], cin.at[0], s_send.at[4], s_recv.at[4], up))
    sums[4].start()
    sums[1].wait_recv()
    comb[1] = raw[1] + bs[before, half:]
    sums.append(copy_to(comb.at[1], cin.at[1], s_send.at[5], s_recv.at[5], down))
    sums[5].start()

    for copy in to_z:
        copy.wait_recv()
    over = copy_to(rall.at[:, c], rall.at[:, c], rc_send.at[0], rc_recv.at[0], partner)
    over.start()
    for copy in sums[2:]:
        copy.wait_recv()
    s_c[:half] = bs[y, :half] + inn[0] + cin[0]
    s_c[half:] = bs[y, half:] + inn[1] + cin[1]
    over.wait_recv()
    for b in range(32):
        rc[b * OWN : (b + 1) * OWN] = rall[b // 2, b % 2]
    pall[y] = jnp.dot(s_c[...], rc[...], precision=highest, preferred_element_type=f32)

    def rows_of(q, h):
        return pall.at[q, pl.ds(half * h, half)]

    gather_ring(rows_of, y, up, down, p_send, p_recv)
    projected = pall[0] + pall[1] + pall[2] + pall[3]
    p_out[...] = projected

    along_rows = (((0,), (0,)), ((), ()))
    gram[...] = lax.dot_general(projected, projected, along_rows, precision=highest, preferred_element_type=f32)
    for g in range(8):
        part = s_c[:, g * FACTOR_ROWS : (g + 1) * FACTOR_ROWS]
        mloc[g, :FACTOR_ROWS] = lax.dot_general(
            part, projected, along_rows, precision=highest, preferred_element_type=f32
        )
        mloc[g, FACTOR_ROWS:] = gram[pl.ds(pl.multiple_of(64 * y + 8 * g, 8), 8), :]

    to_core = copy_to(mloc.at[pl.ds(4 * (1 - c), 4)], crecv, c_send.at[0], c_recv.at[0], partner)
    to_core.start()
    to_core.wait_recv()
    for q in range(4):
        mx[q] = mloc[4 * c + q] + crecv[q]
    sums_x = [
        copy_to(mx.at[(x + d) % 4], xrecv.at[d - 1], x_send.at[d - 1], x_recv.at[d - 1], at_x((x + d) % 4))
        for d in (2, 1, 3)
    ]
    for copy in sums_x:
        copy.start()
    for copy in sums_x:
        copy.wait_recv()
    mz[...] = mx[x] + xrecv[0] + xrecv[1] + xrecv[2]

    owners = [(16 * t + 9) // 10 for t in range(TILES)]
    tile = (z * TILES) // NZ
    owner = (z * TILES) % NZ < TILES
    sums_z = [
        copy_to(mz.at[pl.ds(8 * t, 8)], zrecv.at[z], z_send.at[t], z_recv.at[z], at_z(owners[t]))
        for t in range(TILES)
    ]
    for t in range(TILES):

        @pl.when(z != owners[t])
        def _():
            sums_z[t].start()

    group = 4 * c + x
    rows = pl.ds(pl.multiple_of(8 * tile, 8), 8)
    to_all = [
        copy_to(
            fin, mall.at[y, group, rows], f_send.at[d - 1], f_recv.at[tile], at_z((z + d) % NZ)
        )
        for d in order
    ]

    @pl.when(owner)
    def _():
        zrecv[z] = mz[rows, :]
        for s in range(NZ):

            @pl.when(z != s)
            def _():
                copy_to(zrecv.at[s], zrecv.at[s], z_send.at[0], z_recv.at[s], partner).wait_recv()

        total = zrecv[0]
        for s in range(1, NZ):
            total = total + zrecv[s]
        fin[...] = total
        for copy in to_all:
            copy.start()
        mall[y, group, rows] = total

    for t in range(TILES):

        @pl.when(z != owners[t])
        def _():
            copy_to(
                fin, mall.at[y, group, pl.ds(8 * t, 8)], f_send.at[0], f_recv.at[t], partner
            ).wait_recv()

    east, west = at_x((x + 1) % 4), at_x((x + 3) % 4)

    @pl.when(c == 0)
    def _():
        gather_ring(lambda q, h: mall.at[y, q, pl.ds(40 * h, 40)], x, east, west, a_send, a_recv)
        gather_ring(lambda q, h: mall.at[q, pl.ds(2 * h, 2)], y, up, down, b_send, b_recv)

    @pl.when(c == 1)
    def _():
        gather_ring(lambda q, h: mall.at[q, 4 + x, pl.ds(40 * h, 40)], y, up, down, a_send, a_recv)
        gather_ring(lambda q, h: mall.at[pl.ds(2 * h, 2), 4 + q], x, east, west, b_send, b_recv)

    halves = copy_to(
        mall.at[:, pl.ds(4 * c, 4)], mall.at[:, pl.ds(4 * c, 4)], d_send.at[0], d_recv.at[0], partner
    )
    halves.start()

    @pl.when(source)
    def _():
        for copy in to_x:
            copy.wait_send()

    for copy in to_z + sums + [over, to_core] + sums_x:
        copy.wait_send()
    for t in range(TILES):

        @pl.when(z != owners[t])
        def _():
            sums_z[t].wait_send()

    @pl.when(owner)
    def _():
        for copy in to_all:
            copy.wait_send()

    halves.wait_send()
    halves.wait_recv()


def exchange(momentum, gradient, right_factor):
    sem = pltpu.SemaphoreType.DMA
    half = SHARD // 2
    counts = (3, 6, 6, 3, 1, 15, 15, 1, 1, 6, 6, 1, 1, 3, 3, TILES, NZ, 15, TILES, 6, 6, 6, 6, 1, 1)
    return pl.pallas_call(
        exchange_kernel,
        name="exchange",
        out_shape=(
            jax.ShapeDtypeStruct((SHARD, RANK), f32),
            jax.ShapeDtypeStruct((4, 8, PIECE, RANK), f32),
        ),
        in_specs=[pl.BlockSpec(memory_space=pl.ANY)] * 3,
        out_specs=(pl.BlockSpec(memory_space=VMEM),) * 2,
        scratch_shapes=[
            VMEM((SHARD, COLS), f32),
            VMEM((SHARD, COLS), jnp.bfloat16),
            VMEM((4, SHARD, BLOCK), f32),
            VMEM((2, half, BLOCK), f32),
            VMEM((2, half, BLOCK), f32),
            VMEM((2, half, BLOCK), f32),
            VMEM((2, half, BLOCK), f32),
            VMEM((SHARD, BLOCK), f32),
            VMEM((NZ, 2, OWN, RANK), f32),
            VMEM((BLOCK, RANK), f32),
            VMEM((4, SHARD, RANK), f32),
            VMEM((RANK, RANK), f32),
            VMEM((8, PIECE, RANK), f32),
            VMEM((4, PIECE, RANK), f32),
            VMEM((4, PIECE, RANK), f32),
            VMEM((3, PIECE, RANK), f32),
            VMEM((PIECE, RANK), f32),
            VMEM((NZ, 8, RANK), f32),
            VMEM((8, RANK), f32),
        ]
        + [sem((n,)) for n in counts],
        compiler_params=pltpu.CompilerParams(
            collective_id=0, has_side_effects=True, vmem_limit_bytes=40 * 1024 * 1024
        ),
    )(momentum, gradient, right_factor)


def dot(a, b, contract, precise=True):
    if not precise:
        a, b = a.astype(jnp.bfloat16), b.astype(jnp.bfloat16)
    return lax.dot_general(
        a, b, (contract, ((), ())), precision=highest if precise else None, preferred_element_type=f32
    )


def finish_kernel(m_hbm, g_hbm, p_ref, mall, new_m, update, new_f, mv, gv, a_ref, x_ref, w_ref, fbuf, load):
    load_m = pltpu.make_async_copy(m_hbm.at[0], mv, load.at[0])
    load_g = pltpu.make_async_copy(g_hbm.at[0], gv, load.at[1])
    load_m.start()
    load_g.start()
    x, z, c = (lax.axis_index(name) for name in FSDP)

    for g in range(4):
        for i in range(8):
            a_ref[64 * g + 8 * i : 64 * g + 8 * i + 8, :] = mall[g, i, FACTOR_ROWS:]
    row = lax.broadcasted_iota(jnp.int32, (RANK, RANK), 0)
    col = lax.broadcasted_iota(jnp.int32, (RANK, RANK), 1)
    gram = a_ref[...]
    diagonal = jnp.where(row == col, gram, 0.0)
    by_row = lax.rsqrt(jnp.sum(diagonal, axis=1, keepdims=True))
    by_col = lax.rsqrt(jnp.sum(diagonal, axis=0, keepdims=True))
    scaled = gram * by_row * by_col
    a_ref[...] = scaled
    bound = jnp.max(jnp.sum(jnp.abs(scaled), axis=0, keepdims=True), axis=1, keepdims=True)
    x_ref[...] = jnp.where(row == col, lax.rsqrt(bound / 1.5), 0.0)

    def step(precise):
        def body(state):
            _, count = state
            inverse = x_ref[...]
            error = dot(dot(inverse, a_ref[...], ((1,), (0,)), precise), inverse, ((1,), (1,)), precise)
            error = jnp.where(row == col, error - 1.0, error)
            lower = jnp.where(row > col, error, jnp.where(row == col, 0.5 * error, 0.0))
            x_ref[...] = inverse - dot(lower, inverse, ((1,), (0,)), precise)
            return jnp.sum(error * error), count + 1

        return body

    rough = lax.while_loop(
        lambda s: (s[0] > 0.04) & (s[1] < 12), step(False), (jnp.float32(1e9), jnp.int32(0))
    )
    del rough
    size, _ = lax.while_loop(
        lambda s: (s[0] > 1e-6) & (s[1] < 40), step(True), (jnp.float32(1e9), jnp.int32(0))
    )

    @pl.when(jnp.logical_not(size <= 1e-6))
    def _():
        w_ref[...] = a_ref[...]
        x_ref[...] = jnp.where(row == col, 1.0, 0.0)

        def eliminate(j, carry):
            work = w_ref[...]
            inverse = x_ref[...]
            column = jnp.sum(jnp.where(col == j, work, 0.0), axis=1, keepdims=True)
            line = jnp.sum(jnp.where(row == j, work, 0.0), axis=0, keepdims=True)
            own = jnp.sum(jnp.where(row == j, inverse, 0.0), axis=0, keepdims=True)
            pivot = jnp.max(jnp.where(row[:, :1] == j, column, -jnp.inf), axis=0, keepdims=True)
            ratio = jnp.where(row[:, :1] > j, column / pivot, 0.0)
            w_ref[...] = work - ratio * line
            x_ref[...] = jnp.where(row == j, own / jnp.sqrt(pivot), inverse - ratio * own)
            return carry

        lax.fori_loop(0, RANK, eliminate, 0)

    inverse = jnp.where(row >= col, x_ref[...], 0.0) * by_col
    x_ref[...] = inverse
    squares = jnp.zeros((1, RANK), f32)
    for q in range(4):
        block = mall[q, :, :FACTOR_ROWS].reshape(BLOCK, RANK)
        factor = dot(block, inverse, ((1,), (1,))) * (1.0 / REPLICAS)
        fbuf[q * BLOCK : (q + 1) * BLOCK] = factor
        squares = squares + jnp.sum(factor * factor, axis=0, keepdims=True)
    norms = jnp.sqrt(squares + epsilon)
    orthonormal = dot(p_ref[...], inverse, ((1,), (1,)))
    directions = orthonormal / norms * math.sqrt(ROWS * COLS / RANK)

    place = x * 32 + z * 2 + c
    for j in range(4):

        @pl.when(place % 4 == j)
        def _():
            own = mall[place // 32, (place % 32) // 4, OWN * j : OWN * (j + 1)]
            new_f[...] = dot(own, inverse, ((1,), (1,))) * (1.0 / REPLICAS) / norms

    load_m.wait()
    load_g.wait()
    width = 256
    for j in range(COLS // width):
        columns = slice(j * width, (j + 1) * width)
        factor = fbuf[columns, :]
        correction = dot(orthonormal, factor, ((1,), (1,)))
        new_m[0, :, columns] = mv[:, columns] + gv[:, columns].astype(f32) - (1.0 - decay_rate) * correction
        update[:, columns] = dot(directions, factor, ((1,), (1,))).astype(jnp.bfloat16)


def finish(momentum, gradient, projected, mall):
    vmem = pl.BlockSpec(memory_space=VMEM)
    anywhere = pl.BlockSpec(memory_space=pl.ANY)
    return pl.pallas_call(
        finish_kernel,
        name="finish",
        out_shape=(
            jax.ShapeDtypeStruct((1, SHARD, COLS), f32),
            jax.ShapeDtypeStruct((SHARD, COLS), jnp.bfloat16),
            jax.ShapeDtypeStruct((OWN, RANK), f32),
        ),
        in_specs=[anywhere, anywhere, vmem, vmem],
        out_specs=(vmem,) * 3,
        scratch_shapes=[
            VMEM((SHARD, COLS), f32),
            VMEM((SHARD, COLS), jnp.bfloat16),
            VMEM((RANK, RANK), f32),
            VMEM((RANK, RANK), f32),
            VMEM((RANK, RANK), f32),
            VMEM((COLS, RANK), f32),
            pltpu.SemaphoreType.DMA((2,)),
        ],
        compiler_params=pltpu.CompilerParams(vmem_limit_bytes=40 * 1024 * 1024),
    )(momentum, gradient, projected, mall)


def shards(momentum, gradient, right_factor):
    projected, mall = exchange(momentum, gradient, right_factor)
    return finish(momentum, gradient, projected, mall)


def solution(mesh):
    split = Mesh(mesh.devices.reshape(mesh.shape["rep"], NX, NZ, 2), ("rep",) + FSDP)
    in_specs = (P("rep", FSDP, None), P("rep", FSDP, None), P(FSDP, None))
    out_specs = (P("rep", FSDP, None), P(FSDP, None), P(FSDP, None))
    return jax.shard_map(
        shards, mesh=split, in_specs=in_specs, out_specs=out_specs, check_vma=False
    )
```

```python
import math

import jax
import jax.numpy as jnp
from jax import lax
from jax.experimental import pallas as pl
from jax.experimental.pallas import tpu as pltpu
from jax.sharding import Mesh
from jax.sharding import PartitionSpec as P

ROWS = 18432
COLS = 2304
RANK = 256
REPLICAS = 4
FSDP = ("fx", "fz", "fc")

NX, NZ = 4, 16
SHARD = ROWS // 128
BLOCK = COLS // 4
OWN = COLS // 128
PIECE = 80
FACTOR_ROWS = 72
TILES = PIECE // 8

epsilon = 1e-06
decay_rate = 0.95
highest = lax.Precision.HIGHEST
MESH = pl.DeviceIdType.MESH
VMEM = pltpu.VMEM
f32 = jnp.float32


def copy_to(src, dst, send, recv, device):
    return pltpu.make_async_remote_copy(
        src_ref=src,
        dst_ref=dst,
        send_sem=send,
        recv_sem=recv,
        device_id=device,
        device_id_type=MESH,
    )


def gather_ring(block, me, right, left, send, recv):
    before, after, across = (me + 3) % 4, (me + 1) % 4, (me + 2) % 4

    def hop(q, h, device, i):
        return copy_to(block(q, h), block(q, h), send.at[i], recv.at[i], device)

    first = [hop(me, 0, right, 0), hop(me, 1, left, 1), hop(me, 1, right, 2), hop(me, 0, left, 3)]
    for copy in first:
        copy.start()
    first[0].wait_recv()
    onward = hop(before, 0, right, 4)
    onward.start()
    first[1].wait_recv()
    backward = hop(after, 1, left, 5)
    backward.start()
    first[2].wait_recv()
    first[3].wait_recv()
    onward.wait_recv()
    backward.wait_recv()
    for copy in first + [onward, backward]:
        copy.wait_send()


def exchange_kernel(
    m_hbm, g_hbm, r_hbm, buffer, p_out, mall,
    mv, gv, bs, raw, comb, cin, inn, s_c, s_t, rall, rc, pall, gram, mloc, crecv, mx, xrecv, mz, zrecv, fin,
    load, s_send, s_recv, rx_send, rx_recv, rz_send, rz_recv, rc_send, rc_recv, p_send, p_recv,
    c_send, c_recv, x_send, x_recv, z_send, z_recv, f_send, f_recv, a_send, a_recv, b_send, b_recv,
    d_send, d_recv,
):
    y, x, z, c = (lax.axis_index(name) for name in ("rep",) + FSDP)

    def at_y(q):
        return (q, x, z, c)

    def at_x(q):
        return (y, q, z, c)

    def at_z(q):
        return (y, x, q, c)

    partner = (y, x, z, 1 - c)
    peers = [at_z((z + d) % NZ) for d in sorted(range(1, NZ), key=lambda d: abs(d - NZ // 2))]
    peers += [at_y((y + d) % 4) for d in range(1, 4)]
    peers += [at_x((x + d) % 4) for d in range(1, 4)]
    peers += [partner]
    source = x == y
    load_m = pltpu.make_async_copy(m_hbm.at[0], mv, load.at[0])
    load_g = pltpu.make_async_copy(g_hbm.at[0], gv, load.at[1])
    load_r = pltpu.make_async_copy(r_hbm, rall.at[z, c], load.at[2])

    @pl.when(source)
    def _():
        load_r.start()

    load_m.start()
    load_g.start()
    barrier = pltpu.get_barrier_semaphore()
    for peer in peers:
        pl.semaphore_signal(barrier, inc=1, device_id=peer, device_id_type=MESH)

    load_m.wait()
    load_g.wait()
    for q in range(4):
        columns = slice(q * BLOCK, (q + 1) * BLOCK)
        part = mv[:, columns] + gv[:, columns].astype(f32)
        buffer[:, columns] = part
        bs[q] = part

    @pl.when(source)
    def _():
        load_r.wait()

    pl.semaphore_wait(barrier, len(peers))

    to_x = [
        copy_to(rall.at[z, c], rall.at[z, c], rx_send.at[d - 1], rx_recv.at[0], at_x((x + d) % 4))
        for d in range(1, 4)
    ]

    @pl.when(source)
    def _():
        for copy in to_x:
            copy.start()

    half = SHARD // 2
    up, down = at_y((y + 1) % 4), at_y((y + 3) % 4)
    after, before, across = (y + 1) % 4, (y + 3) % 4, (y + 2) % 4
    low, high = pl.ds(0, half), pl.ds(half, half)
    sums = [
        copy_to(bs.at[across, low], raw.at[0], s_send.at[0], s_recv.at[0], up),
        copy_to(bs.at[across, high], raw.at[1], s_send.at[1], s_recv.at[1], down),
        copy_to(bs.at[after, high], inn.at[1], s_send.at[2], s_recv.at[2], up),
        copy_to(bs.at[before, low], inn.at[0], s_send.at[3], s_recv.at[3], down),
    ]
    for copy in sums:
        copy.start()

    @pl.when(jnp.logical_not(source))
    def _():
        to_x[0].wait_recv()

    def along_z(owner, far, step):
        block = rall.at[(z + NZ - owner) % NZ, c]
        return copy_to(block, block, rz_send.at[far % NZ - 1], rz_recv.at[far % NZ - 1], at_z((z + NZ + step) % NZ))

    to_z = [along_z(0, d, d) for d in (4, -4, 3, -3, 2, -2, 1, -1)]
    for copy in to_z:
        copy.start()

    sums[0].wait_recv()
    comb[0] = raw[0] + bs[after, :half]
    sums.append(copy_to(comb.at[0], cin.at[0], s_send.at[4], s_recv.at[4], up))
    sums[4].start()
    sums[1].wait_recv()
    comb[1] = raw[1] + bs[before, half:]
    sums.append(copy_to(comb.at[1], cin.at[1], s_send.at[5], s_recv.at[5], down))
    sums[5].start()

    to_z[0].wait_recv()
    beyond = [along_z(4, 4 + d, d) for d in (4, 3, 2, 1)]
    for copy in beyond:
        copy.start()
    to_z[1].wait_recv()
    beyond += [along_z(-4, -4 - d, -d) for d in (3, 2, 1)]
    for copy in beyond[4:]:
        copy.start()

    for copy in sums[2:]:
        copy.wait_recv()
    s_c[:half] = bs[y, :half] + inn[0] + cin[0]
    s_c[half:] = bs[y, half:] + inn[1] + cin[1]
    s_t[...] = s_c[...].T

    for copy in to_z[2:] + beyond:
        copy.wait_recv()
    over = copy_to(rall.at[:, c], rall.at[:, c], rc_send.at[0], rc_recv.at[0], partner)
    over.start()
    over.wait_recv()
    for b in range(32):
        rc[b * OWN : (b + 1) * OWN] = rall[b // 2, b % 2]
    pall[y] = jnp.dot(s_c[...], rc[...], precision=highest, preferred_element_type=f32)

    def rows_of(q, h):
        return pall.at[q, pl.ds(half * h, half)]

    gather_ring(rows_of, y, up, down, p_send, p_recv)
    projected = pall[0] + pall[1] + pall[2] + pall[3]
    p_out[...] = projected

    along_rows = (((0,), (0,)), ((), ()))
    gram[...] = lax.dot_general(projected, projected, along_rows, precision=highest, preferred_element_type=f32)

    def fill(side):
        rows = pl.ds(pl.multiple_of(4 * FACTOR_ROWS * side, 8), 4 * FACTOR_ROWS)
        part = jnp.dot(s_t[rows, :], projected, precision=highest, preferred_element_type=f32)
        for i in range(4):
            mloc[4 * side + i, :FACTOR_ROWS] = part[i * FACTOR_ROWS : (i + 1) * FACTOR_ROWS]
            mloc[4 * side + i, FACTOR_ROWS:] = gram[
                pl.ds(pl.multiple_of(64 * y + 8 * (4 * side + i), 8), 8), :
            ]

    fill(1 - c)
    to_core = copy_to(mloc.at[pl.ds(4 * (1 - c), 4)], crecv, c_send.at[0], c_recv.at[0], partner)
    to_core.start()
    fill(c)
    to_core.wait_recv()
    sums_x = [
        copy_to(mx.at[(x + d) % 4], xrecv.at[d - 1], x_send.at[d - 1], x_recv.at[d - 1], at_x((x + d) % 4))
        for d in (2, 1, 3)
    ]
    for d, copy in zip((2, 1, 3), sums_x, strict=True):
        q = (x + d) % 4
        mx[q] = mloc[4 * c + q] + crecv[q]
        copy.start()
    mx[x] = mloc[4 * c + x] + crecv[x]
    for copy in sums_x:
        copy.wait_recv()
    mz[...] = mx[x] + xrecv[0] + xrecv[1] + xrecv[2]

    owners = [(16 * t + 9) // 10 for t in range(TILES)]
    tile = (z * TILES) // NZ
    owner = (z * TILES) % NZ < TILES
    sums_z = [
        copy_to(mz.at[pl.ds(8 * t, 8)], zrecv.at[z], z_send.at[t], z_recv.at[z], at_z(owners[t]))
        for t in range(TILES)
    ]
    for t in range(TILES):

        @pl.when(z != owners[t])
        def _():
            sums_z[t].start()

    group = 4 * c + x
    rows = pl.ds(pl.multiple_of(8 * tile, 8), 8)
    to_all = [
        copy_to(
            fin, mall.at[y, group, rows], f_send.at[d - 1], f_recv.at[tile], at_z((z + d) % NZ)
        )
        for d in sorted(range(1, NZ), key=lambda d: abs(d - NZ // 2))
    ]

    @pl.when(owner)
    def _():
        zrecv[z] = mz[rows, :]
        for s in range(NZ):

            @pl.when(z != s)
            def _():
                copy_to(zrecv.at[s], zrecv.at[s], z_send.at[0], z_recv.at[s], partner).wait_recv()

        total = zrecv[0]
        for s in range(1, NZ):
            total = total + zrecv[s]
        fin[...] = total
        for copy in to_all:
            copy.start()
        mall[y, group, rows] = total

    for t in range(TILES):

        @pl.when(z != owners[t])
        def _():
            copy_to(
                fin, mall.at[y, group, pl.ds(8 * t, 8)], f_send.at[0], f_recv.at[t], partner
            ).wait_recv()

    first, second = x * (1 - c) + y * c, y * (1 - c) + x * c

    def turned(a, b):
        return (b * (1 - c) + a * c, a * (1 - c) + b * c)

    def block_of(k, j):
        at, to = turned((first + k) % 4, (second + j) % 4)
        return mall.at[at, 4 * c + to]

    def half_of(k, j, h):
        at, to = turned((first + k) % 4, (second + j) % 4)
        return mall.at[at, 4 * c + to, pl.ds(h * (PIECE // 2), PIECE // 2)]

    def on_first(k, h, step, i):
        device = turned((first + step) % 4, second) + (z, c)
        return copy_to(half_of(k, 0, h), half_of(k, 0, h), a_send.at[i], a_recv.at[i], device)

    def on_second(k, j, h, step, i):
        device = turned(first, (second + step) % 4) + (z, c)
        i = 6 * k + i
        return copy_to(half_of(k, j, h), half_of(k, j, h), b_send.at[i], b_recv.at[i], device)

    def on_chip(k, j):
        i = 4 * k + j
        return copy_to(block_of(k, j), block_of(k, j), d_send.at[i], d_recv.at[i], partner)

    ring = [on_first(0, 0, 1, 0), on_first(0, 1, 3, 1), on_first(0, 1, 1, 2), on_first(0, 0, 3, 3)]
    ring += [on_first(3, 0, 1, 4), on_first(1, 1, 3, 5)]
    across_ring = [
        [on_second(k, 0, 0, 1, 0), on_second(k, 0, 1, 3, 1), on_second(k, 0, 1, 1, 2)]
        + [on_second(k, 0, 0, 3, 3), on_second(k, 3, 0, 1, 4), on_second(k, 1, 1, 3, 5)]
        for k in range(4)
    ]
    cores = [[on_chip(k, j) for j in range(4)] for k in range(4)]

    def start_half(k, h):
        for i in ((0, 3), (1, 2))[h]:
            across_ring[k][i].start()

    def hand_on(k):
        for i in range(2):
            across_ring[k][i].wait_recv()
            across_ring[k][4 + i].start()

    def complete(k):
        for i in range(2, 6):
            across_ring[k][i].wait_recv()
        for j in range(1, 4):
            cores[k][j].start()

    for copy in ring[:4]:
        copy.start()
    start_half(0, 0)
    start_half(0, 1)
    cores[0][0].start()
    ring[0].wait_recv()
    ring[4].start()
    start_half(3, 0)
    ring[1].wait_recv()
    ring[5].start()
    start_half(1, 1)
    ring[2].wait_recv()
    start_half(3, 1)
    ring[3].wait_recv()
    start_half(1, 0)
    cores[3][0].start()
    cores[1][0].start()
    hand_on(0)
    ring[4].wait_recv()
    start_half(2, 0)
    ring[5].wait_recv()
    start_half(2, 1)
    cores[2][0].start()
    hand_on(3)
    hand_on(1)
    complete(0)
    hand_on(2)
    complete(3)
    complete(1)
    complete(2)

    @pl.when(source)
    def _():
        for copy in to_x:
            copy.wait_send()

    for copy in to_z + beyond + sums + [over, to_core] + sums_x + ring:
        copy.wait_send()
    for t in range(TILES):

        @pl.when(z != owners[t])
        def _():
            sums_z[t].wait_send()

    @pl.when(owner)
    def _():
        for copy in to_all:
            copy.wait_send()

    for k in range(4):
        for copy in across_ring[k] + cores[k]:
            copy.wait_send()
    for k in range(4):
        for copy in cores[k]:
            copy.wait_recv()


def exchange(momentum, gradient, right_factor):
    sem = pltpu.SemaphoreType.DMA
    half = SHARD // 2
    counts = (3, 6, 6, 3, 1, 15, 15, 1, 1, 6, 6, 1, 1, 3, 3, TILES, NZ, 15, TILES, 6, 6, 24, 24, 16, 16)
    return pl.pallas_call(
        exchange_kernel,
        name="exchange",
        out_shape=(
            jax.ShapeDtypeStruct((SHARD, COLS), f32),
            jax.ShapeDtypeStruct((SHARD, RANK), f32),
            jax.ShapeDtypeStruct((4, 8, PIECE, RANK), f32),
        ),
        in_specs=[pl.BlockSpec(memory_space=pltpu.HBM)] * 3,
        out_specs=(pl.BlockSpec(memory_space=VMEM),) * 3,
        scratch_shapes=[
            VMEM((SHARD, COLS), f32),
            VMEM((SHARD, COLS), jnp.bfloat16),
            VMEM((4, SHARD, BLOCK), f32),
            VMEM((2, half, BLOCK), f32),
            VMEM((2, half, BLOCK), f32),
            VMEM((2, half, BLOCK), f32),
            VMEM((2, half, BLOCK), f32),
            VMEM((SHARD, BLOCK), f32),
            VMEM((BLOCK, SHARD), f32),
            VMEM((NZ, 2, OWN, RANK), f32),
            VMEM((BLOCK, RANK), f32),
            VMEM((4, SHARD, RANK), f32),
            VMEM((RANK, RANK), f32),
            VMEM((8, PIECE, RANK), f32),
            VMEM((4, PIECE, RANK), f32),
            VMEM((4, PIECE, RANK), f32),
            VMEM((3, PIECE, RANK), f32),
            VMEM((PIECE, RANK), f32),
            VMEM((NZ, 8, RANK), f32),
            VMEM((8, RANK), f32),
        ]
        + [sem((n,)) for n in counts],
        compiler_params=pltpu.CompilerParams(
            collective_id=0, has_side_effects=True, vmem_limit_bytes=40 * 1024 * 1024
        ),
    )(*(pltpu.with_memory_space_constraint(a, pltpu.HBM) for a in (momentum, gradient, right_factor)))


def dot(a, b, contract, precise=True):
    if not precise:
        a, b = a.astype(jnp.bfloat16), b.astype(jnp.bfloat16)
    return lax.dot_general(
        a, b, (contract, ((), ())), precision=highest if precise else None, preferred_element_type=f32
    )


def split(a):
    top = a.astype(jnp.bfloat16)
    return top, (a - top.astype(f32)).astype(jnp.bfloat16)


def dot_split(a, b):
    (a_top, a_rest), (b_top, b_rest) = a, b
    turn = (((1,), (1,)), ((), ()))

    def product(left, right):
        return lax.dot_general(left, right, turn, preferred_element_type=f32)

    return product(a_top, b_top) + (product(a_top, b_rest) + product(a_rest, b_top))


def finish_kernel(
    buffer, p_ref, mall, new_m, update, new_f, a_ref, x_ref, w_ref, top_ref, rest_ref, m_buf, u_buf, m_sem, u_sem
):
    x, z, c = (lax.axis_index(name) for name in FSDP)

    for g in range(4):
        for i in range(8):
            a_ref[64 * g + 8 * i : 64 * g + 8 * i + 8, :] = mall[g, i, FACTOR_ROWS:]
    row = lax.broadcasted_iota(jnp.int32, (RANK, RANK), 0)
    col = lax.broadcasted_iota(jnp.int32, (RANK, RANK), 1)
    gram = a_ref[...]
    diagonal = jnp.where(row == col, gram, 0.0)
    by_row = lax.rsqrt(jnp.sum(diagonal, axis=1, keepdims=True))
    by_col = lax.rsqrt(jnp.sum(diagonal, axis=0, keepdims=True))
    scaled = gram * by_row * by_col
    a_ref[...] = scaled
    bound = jnp.max(jnp.sum(jnp.abs(scaled), axis=0, keepdims=True), axis=1, keepdims=True)
    x_ref[...] = jnp.where(row == col, lax.rsqrt(bound / 1.5), 0.0)

    def step(precise):
        def body(state):
            _, count = state
            inverse = x_ref[...]
            error = dot(dot(inverse, a_ref[...], ((1,), (0,)), precise), inverse, ((1,), (1,)), precise)
            error = jnp.where(row == col, error - 1.0, error)
            lower = jnp.where(row > col, error, jnp.where(row == col, 0.5 * error, 0.0))
            x_ref[...] = inverse - dot(lower, inverse, ((1,), (0,)), precise)
            return jnp.sum(error * error), count + 1

        return body

    rough = lax.while_loop(
        lambda s: (s[0] > 0.04) & (s[1] < 12), step(False), (jnp.float32(1e9), jnp.int32(0))
    )
    del rough
    size, _ = lax.while_loop(
        lambda s: (s[0] > 1e-6) & (s[1] < 40), step(True), (jnp.float32(1e9), jnp.int32(0))
    )

    @pl.when(jnp.logical_not(size <= 1e-6))
    def _():
        w_ref[...] = a_ref[...]
        x_ref[...] = jnp.where(row == col, 1.0, 0.0)

        def eliminate(j, carry):
            work = w_ref[...]
            inverse = x_ref[...]
            column = jnp.sum(jnp.where(col == j, work, 0.0), axis=1, keepdims=True)
            line = jnp.sum(jnp.where(row == j, work, 0.0), axis=0, keepdims=True)
            own = jnp.sum(jnp.where(row == j, inverse, 0.0), axis=0, keepdims=True)
            pivot = jnp.max(jnp.where(row[:, :1] == j, column, -jnp.inf), axis=0, keepdims=True)
            ratio = jnp.where(row[:, :1] > j, column / pivot, 0.0)
            w_ref[...] = work - ratio * line
            x_ref[...] = jnp.where(row == j, own / jnp.sqrt(pivot), inverse - ratio * own)
            return carry

        lax.fori_loop(0, RANK, eliminate, 0)

    inverse = jnp.where(row >= col, x_ref[...], 0.0) * by_col
    x_ref[...] = inverse
    halves = split(inverse)
    squares = jnp.zeros((1, RANK), f32)
    for q in range(4):
        block = mall[q, :, :FACTOR_ROWS].reshape(BLOCK, RANK)
        factor = dot_split(split(block), halves) * (1.0 / REPLICAS)
        top, rest = split(factor)
        top_ref[q * BLOCK : (q + 1) * BLOCK] = top
        rest_ref[q * BLOCK : (q + 1) * BLOCK] = rest
        squares = squares + jnp.sum(factor * factor, axis=0, keepdims=True)
    norms = jnp.sqrt(squares + epsilon)
    orthonormal = dot(p_ref[...], inverse, ((1,), (1,)))
    directions = orthonormal / norms * math.sqrt(ROWS * COLS / RANK)

    place = x * 32 + z * 2 + c
    for j in range(4):

        @pl.when(place % 4 == j)
        def _():
            own = mall[place // 32, (place % 32) // 4, OWN * j : OWN * (j + 1)]
            new_f[...] = dot(own, inverse, ((1,), (1,))) * (1.0 / REPLICAS) / norms

    both = split(jnp.concatenate([orthonormal, directions], axis=0))
    width = 256
    copies = []
    for j in range(COLS // width):
        columns = slice(j * width, (j + 1) * width)
        products = dot_split(both, (top_ref[columns, :], rest_ref[columns, :]))
        m_buf[:, columns] = buffer[:, columns] - (1.0 - decay_rate) * products[:SHARD]
        u_buf[:, columns] = products[SHARD:].astype(jnp.bfloat16)
        part = pl.ds(j * width, width)
        copies.append(pltpu.make_async_copy(m_buf.at[:, part], new_m.at[0, :, part], m_sem.at[j]))
        copies.append(pltpu.make_async_copy(u_buf.at[:, part], update.at[:, part], u_sem.at[j]))
        copies[-2].start()
        copies[-1].start()
    for copy in copies:
        copy.wait()


def finish(buffer, projected, mall):
    vmem = pl.BlockSpec(memory_space=VMEM)
    anywhere = pl.BlockSpec(memory_space=pltpu.HBM)
    return pl.pallas_call(
        finish_kernel,
        name="finish",
        out_shape=(
            jax.ShapeDtypeStruct((1, SHARD, COLS), f32),
            jax.ShapeDtypeStruct((SHARD, COLS), jnp.bfloat16),
            jax.ShapeDtypeStruct((OWN, RANK), f32),
        ),
        in_specs=[vmem] * 3,
        out_specs=(anywhere, anywhere, vmem),
        scratch_shapes=[
            VMEM((RANK, RANK), f32),
            VMEM((RANK, RANK), f32),
            VMEM((RANK, RANK), f32),
            VMEM((COLS, RANK), jnp.bfloat16),
            VMEM((COLS, RANK), jnp.bfloat16),
            VMEM((SHARD, COLS), f32),
            VMEM((SHARD, COLS), jnp.bfloat16),
            pltpu.SemaphoreType.DMA((9,)),
            pltpu.SemaphoreType.DMA((9,)),
        ],
        compiler_params=pltpu.CompilerParams(vmem_limit_bytes=40 * 1024 * 1024),
    )(buffer, projected, mall)


def shards(momentum, gradient, right_factor):
    return finish(*exchange(momentum, gradient, right_factor))


def solution(mesh):
    split = Mesh(mesh.devices.reshape(mesh.shape["rep"], NX, NZ, 2), ("rep",) + FSDP)
    in_specs = (P("rep", FSDP, None), P("rep", FSDP, None), P(FSDP, None))
    out_specs = (P("rep", FSDP, None), P(FSDP, None), P(FSDP, None))
    return jax.shard_map(
        shards, mesh=split, in_specs=in_specs, out_specs=out_specs, check_vma=False
    )
```

```python
import math

import jax
import jax.numpy as jnp
from jax import lax
from jax.experimental import pallas as pl
from jax.experimental.pallas import tpu as pltpu
from jax.sharding import Mesh
from jax.sharding import PartitionSpec as P

ROWS = 18432
COLS = 2304
RANK = 256
REPLICAS = 4
FSDP = ("fx", "fz", "fc")

NX, NZ = 4, 16
SHARD = ROWS // 128
BLOCK = COLS // 4
OWN = COLS // 128
PIECE = 80
FACTOR_ROWS = 72
TILES = PIECE // 8

epsilon = 1e-06
decay_rate = 0.95
highest = lax.Precision.HIGHEST
MESH = pl.DeviceIdType.MESH
VMEM = pltpu.VMEM
f32 = jnp.float32


def copy_to(src, dst, send, recv, device):
    return pltpu.make_async_remote_copy(
        src_ref=src,
        dst_ref=dst,
        send_sem=send,
        recv_sem=recv,
        device_id=device,
        device_id_type=MESH,
    )


def gather_ring(block, me, right, left, send, recv):
    before, after, across = (me + 3) % 4, (me + 1) % 4, (me + 2) % 4

    def hop(q, h, device, i):
        return copy_to(block(q, h), block(q, h), send.at[i], recv.at[i], device)

    first = [hop(me, 0, right, 0), hop(me, 1, left, 1), hop(me, 1, right, 2), hop(me, 0, left, 3)]
    for copy in first:
        copy.start()
    first[0].wait_recv()
    onward = hop(before, 0, right, 4)
    onward.start()
    first[1].wait_recv()
    backward = hop(after, 1, left, 5)
    backward.start()
    first[2].wait_recv()
    first[3].wait_recv()
    onward.wait_recv()
    backward.wait_recv()
    for copy in first + [onward, backward]:
        copy.wait_send()


def dot(a, b, contract, precise=True):
    if not precise:
        a, b = a.astype(jnp.bfloat16), b.astype(jnp.bfloat16)
    return lax.dot_general(
        a, b, (contract, ((), ())), precision=highest if precise else None, preferred_element_type=f32
    )


def positions():
    shape = (RANK, RANK)
    return lax.broadcasted_iota(jnp.int32, shape, 0), lax.broadcasted_iota(jnp.int32, shape, 1)


def invert_start(gram, a_ref, x_ref, scale):
    row, col = positions()
    diagonal = jnp.where(row == col, gram, 0.0)
    by_row = lax.rsqrt(jnp.sum(diagonal, axis=1, keepdims=True))
    by_col = lax.rsqrt(jnp.sum(diagonal, axis=0, keepdims=True))
    scaled = gram * by_row * by_col
    a_ref[...] = scaled
    scale[...] = by_col
    bound = jnp.max(jnp.sum(jnp.abs(scaled), axis=0, keepdims=True), axis=1, keepdims=True)
    x_ref[...] = jnp.where(row == col, lax.rsqrt(bound / 1.5), 0.0)


def invert_step(a_ref, x_ref, precise):
    row, col = positions()
    inverse = x_ref[...]
    error = dot(dot(inverse, a_ref[...], ((1,), (0,)), precise), inverse, ((1,), (1,)), precise)
    error = jnp.where(row == col, error - 1.0, error)
    lower = jnp.where(row > col, error, jnp.where(row == col, 0.5 * error, 0.0))
    x_ref[...] = inverse - dot(lower, inverse, ((1,), (0,)), precise)
    return error


def exchange_kernel(
    m_hbm, g_hbm, r_hbm, buffer, p_out, mall, a_out, x_out, scale,
    mv, gv, bs, raw, comb, cin, inn, s_c, s_t, rall, rc, pall, gram, mloc, crecv, mx, xrecv, mz, zrecv, fin, zall, gall,
    load, s_send, s_recv, rx_send, rx_recv, rz_send, rz_recv, rc_send, rc_recv, p_send, p_recv,
    c_send, c_recv, x_send, x_recv, z_send, z_recv, f_send, f_recv, a_send, a_recv, b_send, b_recv,
    d_send, d_recv, gx_send, gx_recv, gy_send, gy_recv, gc_send, gc_recv,
):
    y, x, z, c = (lax.axis_index(name) for name in ("rep",) + FSDP)

    def at_y(q):
        return (q, x, z, c)

    def at_x(q):
        return (y, q, z, c)

    def at_z(q):
        return (y, x, q, c)

    partner = (y, x, z, 1 - c)
    peers = [at_z((z + NZ + d) % NZ) for d in (4, -4, 3, -3, 2, -2, 1, -1)]
    peers += [at_y((y + d) % 4) for d in range(1, 4)]
    peers += [at_x((x + d) % 4) for d in range(1, 4)]
    peers += [partner]
    source = x == y
    load_m = pltpu.make_async_copy(m_hbm.at[0], mv, load.at[0])
    load_g = pltpu.make_async_copy(g_hbm.at[0], gv, load.at[1])
    load_r = pltpu.make_async_copy(r_hbm, rall.at[z, c], load.at[2])

    @pl.when(source)
    def _():
        load_r.start()

    load_m.start()
    load_g.start()
    barrier = pltpu.get_barrier_semaphore()
    for peer in peers:
        pl.semaphore_signal(barrier, inc=1, device_id=peer, device_id_type=MESH)

    load_m.wait()
    load_g.wait()
    for q in range(4):
        columns = slice(q * BLOCK, (q + 1) * BLOCK)
        part = mv[:, columns] + gv[:, columns].astype(f32)
        buffer[:, columns] = part
        bs[q] = part

    @pl.when(source)
    def _():
        load_r.wait()

    pl.semaphore_wait(barrier, len(peers))

    to_x = [
        copy_to(rall.at[z, c], rall.at[z, c], rx_send.at[d - 1], rx_recv.at[0], at_x((x + d) % 4))
        for d in range(1, 4)
    ]

    @pl.when(source)
    def _():
        for copy in to_x:
            copy.start()

    half = SHARD // 2
    up, down = at_y((y + 1) % 4), at_y((y + 3) % 4)
    after, before, across = (y + 1) % 4, (y + 3) % 4, (y + 2) % 4
    low, high = pl.ds(0, half), pl.ds(half, half)
    sums = [
        copy_to(bs.at[across, low], raw.at[0], s_send.at[0], s_recv.at[0], up),
        copy_to(bs.at[across, high], raw.at[1], s_send.at[1], s_recv.at[1], down),
        copy_to(bs.at[after, high], inn.at[1], s_send.at[2], s_recv.at[2], up),
        copy_to(bs.at[before, low], inn.at[0], s_send.at[3], s_recv.at[3], down),
    ]
    for copy in sums:
        copy.start()

    @pl.when(jnp.logical_not(source))
    def _():
        to_x[0].wait_recv()

    def along_z(owner, far, step):
        block = rall.at[(z + NZ - owner) % NZ, c]
        return copy_to(block, block, rz_send.at[far % NZ - 1], rz_recv.at[far % NZ - 1], at_z((z + NZ + step) % NZ))

    to_z = [along_z(0, d, d) for d in (4, -4, 3, -3, 2, -2, 1, -1)]
    for copy in to_z:
        copy.start()

    sums[0].wait_recv()
    comb[0] = raw[0] + bs[after, :half]
    sums.append(copy_to(comb.at[0], cin.at[0], s_send.at[4], s_recv.at[4], up))
    sums[4].start()
    sums[1].wait_recv()
    comb[1] = raw[1] + bs[before, half:]
    sums.append(copy_to(comb.at[1], cin.at[1], s_send.at[5], s_recv.at[5], down))
    sums[5].start()

    to_z[0].wait_recv()
    beyond = [along_z(4, 4 + d, d) for d in (4, 3, 2, 1)]
    for copy in beyond:
        copy.start()
    to_z[1].wait_recv()
    beyond += [along_z(-4, -4 - d, -d) for d in (3, 2, 1)]
    for copy in beyond[4:]:
        copy.start()

    for copy in sums[2:]:
        copy.wait_recv()
    s_c[:half] = bs[y, :half] + inn[0] + cin[0]
    s_c[half:] = bs[y, half:] + inn[1] + cin[1]
    s_t[...] = s_c[...].T

    for copy in to_z[2:] + beyond:
        copy.wait_recv()
    over = copy_to(rall.at[:, c], rall.at[:, c], rc_send.at[0], rc_recv.at[0], partner)
    over.start()
    over.wait_recv()
    for b in range(32):
        rc[b * OWN : (b + 1) * OWN] = rall[b // 2, b % 2]
    pall[y] = jnp.dot(s_c[...], rc[...], precision=highest, preferred_element_type=f32)

    def rows_of(q, h):
        return pall.at[q, pl.ds(half * h, half)]

    gather_ring(rows_of, y, up, down, p_send, p_recv)
    projected = pall[0] + pall[1] + pall[2] + pall[3]
    p_out[...] = projected

    along_rows = (((0,), (0,)), ((), ()))
    gram[...] = lax.dot_general(projected, projected, along_rows, precision=highest, preferred_element_type=f32)

    def fill(side):
        rows = pl.ds(pl.multiple_of(4 * FACTOR_ROWS * side, 8), 4 * FACTOR_ROWS)
        part = jnp.dot(s_t[rows, :], projected, precision=highest, preferred_element_type=f32)
        for i in range(4):
            mloc[4 * side + i, :FACTOR_ROWS] = part[i * FACTOR_ROWS : (i + 1) * FACTOR_ROWS]
            mloc[4 * side + i, FACTOR_ROWS:] = gram[
                pl.ds(pl.multiple_of(64 * y + 8 * (4 * side + i), 8), 8), :
            ]

    fill(1 - c)
    to_core = copy_to(mloc.at[pl.ds(4 * (1 - c), 4)], crecv, c_send.at[0], c_recv.at[0], partner)
    to_core.start()
    fill(c)
    to_core.wait_recv()
    sums_x = [
        copy_to(mx.at[(x + d) % 4], xrecv.at[d - 1], x_send.at[d - 1], x_recv.at[d - 1], at_x((x + d) % 4))
        for d in (2, 1, 3)
    ]
    for d, copy in zip((2, 1, 3), sums_x, strict=True):
        q = (x + d) % 4
        mx[q] = mloc[4 * c + q] + crecv[q]
        copy.start()
    mx[x] = mloc[4 * c + x] + crecv[x]
    for copy in sums_x:
        copy.wait_recv()
    mz[...] = mx[x] + xrecv[0] + xrecv[1] + xrecv[2]

    owners = [(16 * t + 9) // 10 for t in range(TILES)]
    tile = (z * TILES) // NZ
    owner = (z * TILES) % NZ < TILES
    sums_z = [
        copy_to(mz.at[pl.ds(8 * t, 8)], zrecv.at[z], z_send.at[t], z_recv.at[z], at_z(owners[t]))
        for t in range(TILES)
    ]
    for t in range(TILES):

        @pl.when(z != owners[t])
        def _():
            sums_z[t].start()

    group = 4 * c + x
    rows = pl.ds(pl.multiple_of(8 * tile, 8), 8)
    to_all = [
        copy_to(
            fin, zall.at[rows], f_send.at[d - 1], f_recv.at[tile], at_z((z + d) % NZ)
        )
        for d in sorted(range(1, NZ), key=lambda d: abs(d - NZ // 2))
    ]

    @pl.when(owner)
    def _():
        zrecv[z] = mz[rows, :]
        for s in range(NZ):

            @pl.when(z != s)
            def _():
                copy_to(zrecv.at[s], zrecv.at[s], z_send.at[0], z_recv.at[s], partner).wait_recv()

        total = zrecv[0]
        for s in range(1, NZ):
            total = total + zrecv[s]
        fin[...] = total
        for copy in to_all:
            copy.start()
        zall[rows, :] = total

    def tile_here(t):
        @pl.when(z != owners[t])
        def _():
            copy_to(fin, zall.at[pl.ds(8 * t, 8)], f_send.at[0], f_recv.at[t], partner).wait_recv()

    tile_here(TILES - 1)
    gram_rows = pl.ds(FACTOR_ROWS, 8)
    gram_x = [
        copy_to(
            zall.at[gram_rows], gall.at[y, group], gx_send.at[d - 1], gx_recv.at[d - 1], at_x((x + d) % 4)
        )
        for d in (2, 1, 3)
    ]
    mine = pl.ds(4 * c, 4)
    gram_y = [
        copy_to(gall.at[y, mine], gall.at[y, mine], gy_send.at[d - 1], gy_recv.at[d - 1], at_y((y + d) % 4))
        for d in (2, 1, 3)
    ]
    gram_core = copy_to(gall.at[:, mine], gall.at[:, mine], gc_send.at[0], gc_recv.at[0], partner)
    for copy in gram_x:
        copy.start()
    gall[y, group] = zall[gram_rows, :]
    for t in range(TILES - 1):
        tile_here(t)

    first, second = x * (1 - c) + y * c, y * (1 - c) + x * c

    def turned(a, b):
        return (b * (1 - c) + a * c, a * (1 - c) + b * c)

    def block_of(k, j):
        at, to = turned((first + k) % 4, (second + j) % 4)
        return mall.at[at, 4 * c + to]

    def half_of(k, j, h):
        at, to = turned((first + k) % 4, (second + j) % 4)
        return mall.at[at, 4 * c + to, pl.ds(40 * h, 40 - 8 * h)]

    def source_of(k, j, h):
        return half_of(k, j, h) if k or j else zall.at[pl.ds(40 * h, 40 - 8 * h)]

    def on_first(k, h, step, i):
        device = turned((first + step) % 4, second) + (z, c)
        return copy_to(source_of(k, 0, h), half_of(k, 0, h), a_send.at[i], a_recv.at[i], device)

    def on_second(k, j, h, step, i):
        device = turned(first, (second + step) % 4) + (z, c)
        i = 6 * k + i
        return copy_to(source_of(k, j, h), half_of(k, j, h), b_send.at[i], b_recv.at[i], device)

    def on_chip(k, j):
        i = 4 * k + j
        source = block_of(k, j) if k or j else zall.at[pl.ds(0, FACTOR_ROWS)]
        return copy_to(source, block_of(k, j), d_send.at[i], d_recv.at[i], partner)

    ring = [on_first(0, 0, 1, 0), on_first(0, 1, 3, 1), on_first(0, 1, 1, 2), on_first(0, 0, 3, 3)]
    ring += [on_first(3, 0, 1, 4), on_first(1, 1, 3, 5)]
    across_ring = [
        [on_second(k, 0, 0, 1, 0), on_second(k, 0, 1, 3, 1), on_second(k, 0, 1, 1, 2)]
        + [on_second(k, 0, 0, 3, 3), on_second(k, 3, 0, 1, 4), on_second(k, 1, 1, 3, 5)]
        for k in range(4)
    ]
    cores = [[on_chip(k, j) for j in range(4)] for k in range(4)]

    def start_half(k, h):
        for i in ((0, 3), (1, 2))[h]:
            across_ring[k][i].start()

    def hand_on(k):
        for i in range(2):
            across_ring[k][i].wait_recv()
            across_ring[k][4 + i].start()

    def complete(k):
        for i in range(2, 6):
            across_ring[k][i].wait_recv()
        for j in range(1, 4):
            cores[k][j].start()

    for copy in ring[:4]:
        copy.start()
    start_half(0, 0)
    start_half(0, 1)
    cores[0][0].start()
    mall[y, group] = zall[:FACTOR_ROWS, :]
    for copy in gram_x:
        copy.wait_recv()
    for copy in gram_y:
        copy.start()
    ring[0].wait_recv()
    ring[4].start()
    start_half(3, 0)
    ring[1].wait_recv()
    ring[5].start()
    start_half(1, 1)
    ring[2].wait_recv()
    start_half(3, 1)
    ring[3].wait_recv()
    start_half(1, 0)
    cores[3][0].start()
    cores[1][0].start()
    for copy in gram_y:
        copy.wait_recv()
    gram_core.start()
    hand_on(0)
    ring[4].wait_recv()
    start_half(2, 0)
    ring[5].wait_recv()
    start_half(2, 1)
    cores[2][0].start()
    hand_on(3)
    hand_on(1)
    gram_core.wait_recv()
    invert_start(gall[...].reshape(RANK, RANK), a_out, x_out, scale)
    invert_step(a_out, x_out, False)
    invert_step(a_out, x_out, False)
    complete(0)
    invert_step(a_out, x_out, False)
    hand_on(2)
    invert_step(a_out, x_out, False)
    invert_step(a_out, x_out, False)
    complete(3)
    invert_step(a_out, x_out, False)
    complete(1)
    invert_step(a_out, x_out, False)
    invert_step(a_out, x_out, True)
    complete(2)

    @pl.when(source)
    def _():
        for copy in to_x:
            copy.wait_send()

    for copy in to_z + beyond + sums + [over, to_core, gram_core] + sums_x + ring + gram_x + gram_y:
        copy.wait_send()
    for t in range(TILES):

        @pl.when(z != owners[t])
        def _():
            sums_z[t].wait_send()

    @pl.when(owner)
    def _():
        for copy in to_all:
            copy.wait_send()

    for k in range(4):
        for copy in across_ring[k] + cores[k]:
            copy.wait_send()
    for k in range(4):
        for copy in cores[k]:
            copy.wait_recv()


def exchange(momentum, gradient, right_factor):
    sem = pltpu.SemaphoreType.DMA
    half = SHARD // 2
    counts = (3, 6, 6, 3, 1, 15, 15, 1, 1, 6, 6, 1, 1, 3, 3, TILES, NZ, 15, TILES, 6, 6, 24, 24, 16, 16, 3, 3, 3, 3, 1, 1)
    return pl.pallas_call(
        exchange_kernel,
        name="exchange",
        out_shape=(
            jax.ShapeDtypeStruct((SHARD, COLS), f32),
            jax.ShapeDtypeStruct((SHARD, RANK), f32),
            jax.ShapeDtypeStruct((4, 8, FACTOR_ROWS, RANK), f32),
            jax.ShapeDtypeStruct((RANK, RANK), f32),
            jax.ShapeDtypeStruct((RANK, RANK), f32),
            jax.ShapeDtypeStruct((1, RANK), f32),
        ),
        in_specs=[pl.BlockSpec(memory_space=pltpu.HBM)] * 3,
        out_specs=(pl.BlockSpec(memory_space=VMEM),) * 6,
        scratch_shapes=[
            VMEM((SHARD, COLS), f32),
            VMEM((SHARD, COLS), jnp.bfloat16),
            VMEM((4, SHARD, BLOCK), f32),
            VMEM((2, half, BLOCK), f32),
            VMEM((2, half, BLOCK), f32),
            VMEM((2, half, BLOCK), f32),
            VMEM((2, half, BLOCK), f32),
            VMEM((SHARD, BLOCK), f32),
            VMEM((BLOCK, SHARD), f32),
            VMEM((NZ, 2, OWN, RANK), f32),
            VMEM((BLOCK, RANK), f32),
            VMEM((4, SHARD, RANK), f32),
            VMEM((RANK, RANK), f32),
            VMEM((8, PIECE, RANK), f32),
            VMEM((4, PIECE, RANK), f32),
            VMEM((4, PIECE, RANK), f32),
            VMEM((3, PIECE, RANK), f32),
            VMEM((PIECE, RANK), f32),
            VMEM((NZ, 8, RANK), f32),
            VMEM((8, RANK), f32),
            VMEM((PIECE, RANK), f32),
            VMEM((4, 8, 8, RANK), f32),
        ]
        + [sem((n,)) for n in counts],
        compiler_params=pltpu.CompilerParams(
            collective_id=0, has_side_effects=True, vmem_limit_bytes=40 * 1024 * 1024
        ),
    )(*(pltpu.with_memory_space_constraint(a, pltpu.HBM) for a in (momentum, gradient, right_factor)))


def split(a):
    top = a.astype(jnp.bfloat16)
    return top, (a - top.astype(f32)).astype(jnp.bfloat16)


def dot_split(a, b):
    (a_top, a_rest), (b_top, b_rest) = a, b
    turn = (((1,), (1,)), ((), ()))

    def product(left, right):
        return lax.dot_general(left, right, turn, preferred_element_type=f32)

    return product(a_top, b_top) + (product(a_top, b_rest) + product(a_rest, b_top))


def finish_kernel(
    buffer, p_ref, mall, a_ref, x_first, scale, new_m, update, new_f,
    x_ref, w_ref, top_ref, rest_ref, m_buf, u_buf, m_sem, u_sem,
):
    x, z, c = (lax.axis_index(name) for name in FSDP)

    row, col = positions()
    x_ref[...] = x_first[...]

    def again(state):
        error = invert_step(a_ref, x_ref, True)
        return jnp.sum(error * error), state[1] + 1

    size, _ = lax.while_loop(
        lambda s: (s[0] > 3e-5) & (s[1] < 40), again, (jnp.float32(1e9), jnp.int32(0))
    )

    @pl.when(jnp.logical_not(size <= 3e-5))
    def _():
        w_ref[...] = a_ref[...]
        x_ref[...] = jnp.where(row == col, 1.0, 0.0)

        def eliminate(j, carry):
            work = w_ref[...]
            inverse = x_ref[...]
            column = jnp.sum(jnp.where(col == j, work, 0.0), axis=1, keepdims=True)
            line = jnp.sum(jnp.where(row == j, work, 0.0), axis=0, keepdims=True)
            own = jnp.sum(jnp.where(row == j, inverse, 0.0), axis=0, keepdims=True)
            pivot = jnp.max(jnp.where(row[:, :1] == j, column, -jnp.inf), axis=0, keepdims=True)
            ratio = jnp.where(row[:, :1] > j, column / pivot, 0.0)
            w_ref[...] = work - ratio * line
            x_ref[...] = jnp.where(row == j, own / jnp.sqrt(pivot), inverse - ratio * own)
            return carry

        lax.fori_loop(0, RANK, eliminate, 0)

    inverse = jnp.where(row >= col, x_ref[...], 0.0) * scale[...]
    x_ref[...] = inverse
    halves = split(inverse)
    squares = jnp.zeros((1, RANK), f32)
    for q in range(4):
        block = mall[q].reshape(BLOCK, RANK)
        factor = dot_split(split(block), halves) * (1.0 / REPLICAS)
        top, rest = split(factor)
        top_ref[q * BLOCK : (q + 1) * BLOCK] = top
        rest_ref[q * BLOCK : (q + 1) * BLOCK] = rest
        squares = squares + jnp.sum(factor * factor, axis=0, keepdims=True)
    norms = jnp.sqrt(squares + epsilon)
    orthonormal = dot(p_ref[...], inverse, ((1,), (1,)))
    directions = orthonormal / norms * math.sqrt(ROWS * COLS / RANK)

    place = x * 32 + z * 2 + c
    for j in range(4):

        @pl.when(place % 4 == j)
        def _():
            own = mall[place // 32, (place % 32) // 4, OWN * j : OWN * (j + 1)]
            new_f[...] = dot(own, inverse, ((1,), (1,))) * (1.0 / REPLICAS) / norms

    both = split(jnp.concatenate([orthonormal, directions], axis=0))
    width = 256
    copies = []
    for j in range(COLS // width):
        columns = slice(j * width, (j + 1) * width)
        products = dot_split(both, (top_ref[columns, :], rest_ref[columns, :]))
        m_buf[:, columns] = buffer[:, columns] - (1.0 - decay_rate) * products[:SHARD]
        u_buf[:, columns] = products[SHARD:].astype(jnp.bfloat16)
        part = pl.ds(j * width, width)
        copies.append(pltpu.make_async_copy(m_buf.at[:, part], new_m.at[0, :, part], m_sem.at[j]))
        copies.append(pltpu.make_async_copy(u_buf.at[:, part], update.at[:, part], u_sem.at[j]))
        copies[-2].start()
        copies[-1].start()
    for copy in copies:
        copy.wait()


def finish(*gathered):
    vmem = pl.BlockSpec(memory_space=VMEM)
    anywhere = pl.BlockSpec(memory_space=pltpu.HBM)
    return pl.pallas_call(
        finish_kernel,
        name="finish",
        out_shape=(
            jax.ShapeDtypeStruct((1, SHARD, COLS), f32),
            jax.ShapeDtypeStruct((SHARD, COLS), jnp.bfloat16),
            jax.ShapeDtypeStruct((OWN, RANK), f32),
        ),
        in_specs=[vmem] * 6,
        out_specs=(anywhere, anywhere, vmem),
        scratch_shapes=[
            VMEM((RANK, RANK), f32),
            VMEM((RANK, RANK), f32),
            VMEM((COLS, RANK), jnp.bfloat16),
            VMEM((COLS, RANK), jnp.bfloat16),
            VMEM((SHARD, COLS), f32),
            VMEM((SHARD, COLS), jnp.bfloat16),
            pltpu.SemaphoreType.DMA((9,)),
            pltpu.SemaphoreType.DMA((9,)),
        ],
        compiler_params=pltpu.CompilerParams(vmem_limit_bytes=40 * 1024 * 1024),
    )(*gathered)


def shards(momentum, gradient, right_factor):
    return finish(*exchange(momentum, gradient, right_factor))


def solution(mesh):
    split = Mesh(mesh.devices.reshape(mesh.shape["rep"], NX, NZ, 2), ("rep",) + FSDP)
    in_specs = (P("rep", FSDP, None), P("rep", FSDP, None), P(FSDP, None))
    out_specs = (P("rep", FSDP, None), P(FSDP, None), P(FSDP, None))
    return jax.shard_map(
        shards, mesh=split, in_specs=in_specs, out_specs=out_specs, check_vma=False
    )
```

```python
import math

import jax
import jax.numpy as jnp
from jax import lax
from jax.experimental import pallas as pl
from jax.experimental.pallas import tpu as pltpu
from jax.sharding import Mesh
from jax.sharding import PartitionSpec as P

ROWS = 18432
COLS = 2304
RANK = 256
REPLICAS = 4
FSDP = ("fx", "fz", "fc")

NX, NZ = 4, 16
SHARD = ROWS // 128
BLOCK = COLS // 4
PACKED = SHARD * BLOCK // 128
OWN = COLS // 128
PIECE = 80
FACTOR_ROWS = 72
TILES = PIECE // 8

epsilon = 1e-06
decay_rate = 0.95
highest = lax.Precision.HIGHEST
MESH = pl.DeviceIdType.MESH
VMEM = pltpu.VMEM
f32 = jnp.float32


def copy_to(src, dst, send, recv, device):
    return pltpu.make_async_remote_copy(
        src_ref=src,
        dst_ref=dst,
        send_sem=send,
        recv_sem=recv,
        device_id=device,
        device_id_type=MESH,
    )


def took(ref, sem, device):
    copy_to(ref, ref, sem, sem, device).wait_recv()


def gather_ring(block, two, three, me, right, left, send, recv, meanwhile):
    before, after = (me + 3) % 4, (me + 1) % 4

    def hop(q, h, device, i):
        return copy_to(block(q, h), block(q, h), send.at[0], recv.at[i], device)

    first = [hop(me, 0, right, 0), hop(me, 1, left, 1), hop(me, 1, right, 2), hop(me, 0, left, 2)]
    for copy in first:
        copy.start()
    meanwhile()
    first[0].wait_recv()
    hop(before, 0, right, 2).start()
    first[1].wait_recv()
    hop(after, 1, left, 2).start()
    took(two, recv.at[2], right)
    took(three, send.at[0], right)


def dot(a, b, contract, precise=True):
    if not precise:
        a, b = a.astype(jnp.bfloat16), b.astype(jnp.bfloat16)
    return lax.dot_general(
        a, b, (contract, ((), ())), precision=highest if precise else None, preferred_element_type=f32
    )


def positions():
    shape = (RANK, RANK)
    return lax.broadcasted_iota(jnp.int32, shape, 0), lax.broadcasted_iota(jnp.int32, shape, 1)


def invert_start(gram, a_ref, x_ref, scale):
    row, col = positions()
    diagonal = jnp.where(row == col, gram, 0.0)
    by_row = lax.rsqrt(jnp.sum(diagonal, axis=1, keepdims=True))
    by_col = lax.rsqrt(jnp.sum(diagonal, axis=0, keepdims=True))
    scaled = gram * by_row * by_col
    a_ref[...] = scaled
    scale[...] = by_col
    bound = jnp.max(jnp.sum(jnp.abs(scaled), axis=0, keepdims=True), axis=1, keepdims=True)
    x_ref[...] = jnp.where(row == col, lax.rsqrt(bound / 1.5), 0.0)


def invert_step(a_ref, x_ref, precise):
    row, col = positions()
    inverse = x_ref[...]
    error = dot(dot(inverse, a_ref[...], ((1,), (0,)), precise), inverse, ((1,), (1,)), precise)
    error = jnp.where(row == col, error - 1.0, error)
    lower = jnp.where(row > col, error, jnp.where(row == col, 0.5 * error, 0.0))
    x_ref[...] = inverse - dot(lower, inverse, ((1,), (0,)), precise)
    return error


def exchange_kernel(
    m_hbm, g_hbm, r_hbm, buffer, p_out, mall, a_out, x_out, scale, size,
    mv, gv, bs, raw, comb, cin, inn, packed, s_c, s_t, rall, rc, pall, p_t, mloc, crecv, mx, xrecv, mz, zrecv, fin, zall, gall,
    load, s_send, s_recv, rx_send, rx_recv, rz_send, rz_recv, rc_send, rc_recv, p_send, p_recv,
    c_send, c_recv, x_send, x_recv, z_send, z_recv, f_send, f_recv, a_send, a_recv, b_send, b_recv,
    d_send, d_recv, gx_send, gx_recv, gy_send, gy_recv, gc_send, gc_recv,
):
    y, x, z, c = (lax.axis_index(name) for name in ("rep",) + FSDP)

    def at_y(q):
        return (q, x, z, c)

    def at_x(q):
        return (y, q, z, c)

    def at_z(q):
        return (y, x, q, c)

    partner = (y, x, z, 1 - c)
    peers = [at_z((z + NZ + d) % NZ) for d in (4, -4, 3, -3, 2, -2, 1, -1)]
    peers += [at_y((y + d) % 4) for d in range(1, 4)]
    peers += [at_x((x + d) % 4) for d in range(1, 4)]
    peers += [partner]
    source = x == y
    load_m = pltpu.make_async_copy(m_hbm.at[0], mv, load.at[0])
    load_g = pltpu.make_async_copy(g_hbm.at[0], gv, load.at[1])
    load_r = pltpu.make_async_copy(r_hbm, rall.at[z, c], load.at[2])

    @pl.when(source)
    def _():
        load_r.start()

    load_m.start()
    load_g.start()
    barrier = pltpu.get_barrier_semaphore()
    for peer in peers:
        pl.semaphore_signal(barrier, inc=1, device_id=peer, device_id_type=MESH)

    load_m.wait()
    load_g.wait()
    for q in range(4):
        columns = slice(q * BLOCK, (q + 1) * BLOCK)
        part = mv[:, columns] + gv[:, columns].astype(f32)
        buffer[:, columns] = part
        for t in range(4):
            bs[q, t * SHARD : (t + 1) * SHARD] = part[:, t * 128 : (t + 1) * 128]
        bs[q, 4 * SHARD :, :64] = part[: SHARD // 2, 512:]
        bs[q, 4 * SHARD :, 64:] = part[SHARD // 2 :, 512:]

    @pl.when(source)
    def _():
        load_r.wait()

    pl.semaphore_wait(barrier, len(peers))

    to_x = [
        copy_to(rall.at[z, c], rall.at[z, c], rx_send.at[0], rx_recv.at[0], at_x((x + d) % 4))
        for d in range(1, 4)
    ]

    @pl.when(source)
    def _():
        for copy in to_x:
            copy.start()

    half = SHARD // 2
    cut = PACKED // 2 // 8 * 8
    up, down = at_y((y + 1) % 4), at_y((y + 3) % 4)
    after, before, across = (y + 1) % 4, (y + 3) % 4, (y + 2) % 4
    low, high = pl.ds(0, cut), pl.ds(cut, PACKED - cut)
    rest = pl.ds(0, PACKED - cut)
    sums = [
        copy_to(bs.at[across, low], raw.at[0, low], s_send.at[0], s_recv.at[0], up),
        copy_to(bs.at[across, high], raw.at[1, rest], s_send.at[0], s_recv.at[1], down),
        copy_to(bs.at[after, high], inn.at[1, rest], s_send.at[0], s_recv.at[2], up),
        copy_to(bs.at[before, low], inn.at[0, low], s_send.at[0], s_recv.at[2], down),
    ]
    for copy in sums:
        copy.start()

    @pl.when(jnp.logical_not(source))
    def _():
        to_x[0].wait_recv()

    def along_z(owner, far, step):
        block = rall.at[(z + NZ - owner) % NZ, c]
        arrival = {4: 0, -4: 1}.get(far, 2)
        return copy_to(block, block, rz_send.at[0], rz_recv.at[arrival], at_z((z + NZ + step) % NZ))

    to_z = [along_z(0, d, d) for d in (4, -4, 3, -3, 2, -2, 1, -1)]
    for copy in to_z:
        copy.start()

    sums[0].wait_recv()
    comb[0, :cut] = raw[0, :cut] + bs[after, :cut]
    sums.append(copy_to(comb.at[0, low], cin.at[0, low], s_send.at[0], s_recv.at[2], up))
    sums[4].start()
    sums[1].wait_recv()
    comb[1, : PACKED - cut] = raw[1, : PACKED - cut] + bs[before, cut:]
    sums.append(copy_to(comb.at[1, rest], cin.at[1, rest], s_send.at[0], s_recv.at[2], down))
    sums[5].start()

    to_z[0].wait_recv()
    beyond = [along_z(4, 4 + d, d) for d in (4, 3, 2, 1)]
    for copy in beyond:
        copy.start()
    to_z[1].wait_recv()
    beyond += [along_z(-4, -4 - d, -d) for d in (3, 2, 1)]
    for copy in beyond[4:]:
        copy.start()

    took(rall.at[pl.ds(0, 13), c], rz_recv.at[2], partner)
    over = copy_to(rall.at[:, c], rall.at[:, c], rc_send.at[0], rc_recv.at[0], partner)
    over.start()
    took(bs.at[pl.ds(0, 2)], s_recv.at[2], up)
    packed[:cut] = bs[y, :cut] + inn[0, :cut] + cin[0, :cut]
    packed[cut:] = bs[y, cut:] + inn[1, : PACKED - cut] + cin[1, : PACKED - cut]
    for t in range(4):
        s_c[:, t * 128 : (t + 1) * 128] = packed[t * SHARD : (t + 1) * SHARD]
    s_c[: SHARD // 2, 512:] = packed[4 * SHARD :, :64]
    s_c[SHARD // 2 :, 512:] = packed[4 * SHARD :, 64:]
    over.wait_recv()
    for b in range(32):
        rc[b * OWN : (b + 1) * OWN] = rall[b // 2, b % 2]
    pall[y] = jnp.dot(s_c[...], rc[...], precision=highest, preferred_element_type=f32)

    def rows_of(q, h):
        return pall.at[q, pl.ds(half * h, half)]

    def turn():
        s_t[...] = s_c[...].T

    gather_ring(
        rows_of, pall.at[pl.ds(0, 2)], pall.at[pl.ds(0, 3)], y, up, down, p_send, p_recv, turn
    )
    projected = pall[0] + pall[1] + pall[2] + pall[3]
    p_out[...] = projected

    p_t[...] = projected.T

    def fill(side):
        wide, narrow = 4 * FACTOR_ROWS, 32
        rows = pl.ds(pl.multiple_of(wide * side, 8), wide)
        gram_rows = pl.ds(pl.multiple_of(2 * narrow * y + narrow * side, 8), narrow)
        left = jnp.concatenate([s_t[rows, :], p_t[gram_rows, :]], axis=0)
        part = jnp.dot(left, projected, precision=highest, preferred_element_type=f32)
        for i in range(4):
            mloc[4 * side + i, :FACTOR_ROWS] = part[i * FACTOR_ROWS : (i + 1) * FACTOR_ROWS]
            mloc[4 * side + i, FACTOR_ROWS:] = part[wide + 8 * i : wide + 8 * i + 8]

    fill(1 - c)
    to_core = copy_to(mloc.at[pl.ds(4 * (1 - c), 4)], crecv, c_send.at[0], c_recv.at[0], partner)
    to_core.start()
    fill(c)
    to_core.wait_recv()
    factor_rows, gram_rows = pl.ds(0, FACTOR_ROWS), pl.ds(FACTOR_ROWS, 8)

    def along_x(d, part, i):
        q = (x + d) % 4
        return copy_to(mx.at[q, part], xrecv.at[d - 1, part], x_send.at[0], x_recv.at[i], at_x(q))

    sums_g = [along_x(d, gram_rows, 0) for d in (2, 1, 3)]
    sums_x = [along_x(d, factor_rows, 1) for d in (2, 1, 3)]
    for q in range(4):
        mx[q] = mloc[4 * c + q] + crecv[q]
    for copy in sums_g + sums_x:
        copy.start()

    owners = [(16 * t + 9) // 10 for t in range(TILES)]
    tile = (z * TILES) // NZ
    owner = (z * TILES) % NZ < TILES
    sums_z = [
        copy_to(mz.at[pl.ds(8 * t, 8)], zrecv.at[z], z_send.at[0], z_recv.at[0], at_z(owners[t]))
        for t in range(TILES)
    ]

    def to_owner(t):
        @pl.when(z != owners[t])
        def _():
            sums_z[t].start()

    took(mz.at[pl.ds(0, 24)], x_recv.at[0], partner)
    mz[FACTOR_ROWS:] = (
        mx[x, FACTOR_ROWS:] + xrecv[0, FACTOR_ROWS:] + xrecv[1, FACTOR_ROWS:] + xrecv[2, FACTOR_ROWS:]
    )
    to_owner(TILES - 1)
    took(mall.at[0, pl.ds(0, 3)], x_recv.at[1], partner)
    mz[:FACTOR_ROWS] = (
        mx[x, :FACTOR_ROWS] + xrecv[0, :FACTOR_ROWS] + xrecv[1, :FACTOR_ROWS] + xrecv[2, :FACTOR_ROWS]
    )
    for t in range(TILES - 1):
        to_owner(t)

    group = 4 * c + x
    rows = pl.ds(pl.multiple_of(8 * tile, 8), 8)
    to_all = [
        copy_to(
            fin, zall.at[rows], f_send.at[0], f_recv.at[tile // (TILES - 1)], at_z((z + d) % NZ)
        )
        for d in sorted(range(1, NZ), key=lambda d: abs(d - NZ // 2))
    ]

    @pl.when(owner)
    def _():
        took(zrecv.at[pl.ds(0, NZ - 1)], z_recv.at[0], partner)
        zrecv[z] = mz[rows, :]
        total = zrecv[0]
        for s in range(1, NZ):
            total = total + zrecv[s]
        fin[...] = total
        for copy in to_all:
            copy.start()
        zall[rows, :] = total

    last = owners[-1]

    @pl.when(z != last)
    def _():
        took(fin, f_recv.at[1], partner)

    gram_x = [
        copy_to(
            zall.at[gram_rows], gall.at[y, group], gx_send.at[0], gx_recv.at[0], at_x((x + d) % 4)
        )
        for d in (2, 1, 3)
    ]
    mine = pl.ds(4 * c, 4)
    gram_y = [
        copy_to(gall.at[y, mine], gall.at[y, mine], gy_send.at[0], gy_recv.at[0], at_y((y + d) % 4))
        for d in (2, 1, 3)
    ]
    gram_core = copy_to(gall.at[:, mine], gall.at[:, mine], gc_send.at[0], gc_recv.at[0], partner)
    for copy in gram_x:
        copy.start()
    gall[y, group] = zall[gram_rows, :]
    took(gall.at[y, pl.ds(0, 3)], gx_recv.at[0], partner)
    for copy in gram_y:
        copy.start()
    owns_factor = owner & (z != last)

    @pl.when(owns_factor)
    def _():
        took(zall.at[pl.ds(0, FACTOR_ROWS - 8)], f_recv.at[0], partner)

    @pl.when(jnp.logical_not(owns_factor))
    def _():
        took(zall.at[pl.ds(0, FACTOR_ROWS)], f_recv.at[0], partner)


    first, second = x * (1 - c) + y * c, y * (1 - c) + x * c

    def turned(a, b):
        return (b * (1 - c) + a * c, a * (1 - c) + b * c)

    def block_of(k, j):
        at, to = turned((first + k) % 4, (second + j) % 4)
        return mall.at[at, 4 * c + to]

    def half_of(k, j, h):
        at, to = turned((first + k) % 4, (second + j) % 4)
        return mall.at[at, 4 * c + to, pl.ds(40 * h, 40 - 8 * h)]

    def source_of(k, j, h):
        return half_of(k, j, h) if k or j else zall.at[pl.ds(40 * h, 40 - 8 * h)]

    def on_first(k, h, step, i):
        device = turned((first + step) % 4, second) + (z, c)
        return copy_to(source_of(k, 0, h), half_of(k, 0, h), a_send.at[0], a_recv.at[i], device)

    def on_second(k, j, h, step, i):
        device = turned(first, (second + step) % 4) + (z, c)
        return copy_to(source_of(k, j, h), half_of(k, j, h), b_send.at[0], b_recv.at[3 * k + min(i, 2)], device)

    def on_chip(k, j):
        source = block_of(k, j) if k or j else zall.at[pl.ds(0, FACTOR_ROWS)]
        return copy_to(source, block_of(k, j), d_send.at[0], d_recv.at[0], partner)

    ring = [on_first(0, 0, 1, 0), on_first(0, 1, 3, 1), on_first(0, 1, 1, 2), on_first(0, 0, 3, 3)]
    ring += [on_first(0, 0, 2, 4), on_first(0, 1, 2, 5)]
    across_ring = [
        [on_second(k, 0, 0, 1, 0), on_second(k, 0, 1, 3, 1), on_second(k, 0, 1, 1, 2)]
        + [on_second(k, 0, 0, 3, 3), on_second(k, 3, 0, 1, 4), on_second(k, 1, 1, 3, 5)]
        for k in range(4)
    ]
    cores = [[on_chip(k, j) for j in range(4)] for k in range(4)]

    def start_half(k, h):
        for i in ((0, 3), (1, 2))[h]:
            across_ring[k][i].start()

    def hand_on(k):
        for i in range(2):
            across_ring[k][i].wait_recv()
            across_ring[k][4 + i].start()

    def complete(k):
        took(mall.at[pl.ds(0, 2), 0], b_recv.at[3 * k + 2], partner)
        for j in range(1, 4):
            cores[k][j].start()

    for copy in ring[4:] + ring[:4]:
        copy.start()
    start_half(0, 0)
    start_half(0, 1)
    cores[0][0].start()
    mall[y, group] = zall[:FACTOR_ROWS, :]
    took(gall.at[pl.ds(0, 3), pl.ds(0, 4)], gy_recv.at[0], partner)
    gram_core.start()
    ring[0].wait_recv()
    start_half(3, 0)
    ring[1].wait_recv()
    start_half(1, 1)
    ring[2].wait_recv()
    start_half(3, 1)
    ring[3].wait_recv()
    start_half(1, 0)
    cores[3][0].start()
    cores[1][0].start()
    gram_core.wait_recv()
    invert_start(gall[...].reshape(RANK, RANK), a_out, x_out, scale)
    invert_step(a_out, x_out, False)
    ring[4].wait_recv()
    start_half(2, 0)
    ring[5].wait_recv()
    start_half(2, 1)
    cores[2][0].start()
    hand_on(0)
    for _ in range(2):
        invert_step(a_out, x_out, False)
    hand_on(3)
    hand_on(1)
    for _ in range(2):
        invert_step(a_out, x_out, False)
    hand_on(2)
    complete(0)
    for _ in range(2):
        invert_step(a_out, x_out, False)
    complete(3)
    complete(1)
    invert_step(a_out, x_out, True)
    complete(2)
    error = invert_step(a_out, x_out, True)
    size[...] = jnp.sum(jnp.sum(error * error, axis=0, keepdims=True), axis=1, keepdims=True)

    @pl.when(source)
    def _():
        took(rall.at[pl.ds(0, 3), c], rx_send.at[0], partner)

    took(rall.at[pl.ds(0, 15), c], rz_send.at[0], partner)
    took(bs.at[pl.ds(0, 3)], s_send.at[0], partner)
    over.wait_send()
    to_core.wait_send()
    took(mx.at[pl.ds(0, 3)], x_send.at[0], partner)

    @pl.when(owner)
    def _():
        took(zall.at[pl.ds(0, PIECE - 8)], z_send.at[0], partner)
        took(zrecv.at[pl.ds(0, NZ - 1)], f_send.at[0], partner)

    @pl.when(jnp.logical_not(owner))
    def _():
        took(zall, z_send.at[0], partner)

    took(gall.at[y, pl.ds(0, 3)], gx_send.at[0], partner)
    took(gall.at[pl.ds(0, 3), pl.ds(0, 4)], gy_send.at[0], partner)
    gram_core.wait_send()
    took(mall.at[pl.ds(0, 3), 0], a_send.at[0], partner)
    took(mall.at[pl.ds(0, 3), pl.ds(0, 4)], b_send.at[0], partner)
    took(mall.at[:, pl.ds(0, 4)], d_send.at[0], partner)
    took(mall.at[:, pl.ds(0, 4)], d_recv.at[0], partner)


def exchange(momentum, gradient, right_factor):
    sem = pltpu.SemaphoreType.DMA
    longer = PACKED - PACKED // 2 // 8 * 8
    counts = (3, 1, 3, 1, 1, 1, 3, 1, 1, 1, 3, 1, 1, 1, 2, 1, 1, 1, 2, 1, 6, 1, 12) + (1,) * 8
    return pl.pallas_call(
        exchange_kernel,
        name="exchange",
        out_shape=(
            jax.ShapeDtypeStruct((SHARD, COLS), f32),
            jax.ShapeDtypeStruct((SHARD, RANK), f32),
            jax.ShapeDtypeStruct((4, 8, FACTOR_ROWS, RANK), f32),
            jax.ShapeDtypeStruct((RANK, RANK), f32),
            jax.ShapeDtypeStruct((RANK, RANK), f32),
            jax.ShapeDtypeStruct((1, RANK), f32),
            jax.ShapeDtypeStruct((1, 1), f32),
        ),
        in_specs=[pl.BlockSpec(memory_space=pltpu.HBM)] * 3,
        out_specs=(pl.BlockSpec(memory_space=VMEM),) * 7,
        scratch_shapes=[
            VMEM((SHARD, COLS), f32),
            VMEM((SHARD, COLS), jnp.bfloat16),
            VMEM((4, PACKED, 128), f32),
            VMEM((2, longer, 128), f32),
            VMEM((2, longer, 128), f32),
            VMEM((2, longer, 128), f32),
            VMEM((2, longer, 128), f32),
            VMEM((PACKED, 128), f32),
            VMEM((SHARD, BLOCK), f32),
            VMEM((BLOCK, SHARD), f32),
            VMEM((NZ, 2, OWN, RANK), f32),
            VMEM((BLOCK, RANK), f32),
            VMEM((4, SHARD, RANK), f32),
            VMEM((RANK, SHARD), f32),
            VMEM((8, PIECE, RANK), f32),
            VMEM((4, PIECE, RANK), f32),
            VMEM((4, PIECE, RANK), f32),
            VMEM((3, PIECE, RANK), f32),
            VMEM((PIECE, RANK), f32),
            VMEM((NZ, 8, RANK), f32),
            VMEM((8, RANK), f32),
            VMEM((PIECE, RANK), f32),
            VMEM((4, 8, 8, RANK), f32),
        ]
        + [sem((n,)) for n in counts],
        compiler_params=pltpu.CompilerParams(
            collective_id=0, has_side_effects=True, vmem_limit_bytes=40 * 1024 * 1024
        ),
    )(*(pltpu.with_memory_space_constraint(a, pltpu.HBM) for a in (momentum, gradient, right_factor)))


def split(a):
    top = a.astype(jnp.bfloat16)
    return top, (a - top.astype(f32)).astype(jnp.bfloat16)


def dot_split(a, b):
    (a_top, a_rest), (b_top, b_rest) = a, b
    turn = (((1,), (1,)), ((), ()))

    def product(left, right):
        return lax.dot_general(left, right, turn, preferred_element_type=f32)

    return product(a_top, b_top) + (product(a_top, b_rest) + product(a_rest, b_top))


def finish_kernel(
    buffer, p_ref, mall, a_ref, x_first, scale, first_size, new_m, update, new_f,
    x_ref, w_ref, top_ref, rest_ref, m_buf, u_buf, m_sem, u_sem,
):
    x, z, c = (lax.axis_index(name) for name in FSDP)

    row, col = positions()
    x_ref[...] = x_first[...]

    def again(state):
        error = invert_step(a_ref, x_ref, True)
        return jnp.sum(error * error), state[1] + 1

    size, _ = lax.while_loop(
        lambda s: jnp.logical_not(s[0] <= 3e-5) & (s[1] < 40), again, (jnp.max(first_size[...]), jnp.int32(0))
    )

    @pl.when(jnp.logical_not(size <= 3e-5))
    def _():
        w_ref[...] = a_ref[...]
        x_ref[...] = jnp.where(row == col, 1.0, 0.0)

        def eliminate(j, carry):
            work = w_ref[...]
            inverse = x_ref[...]
            column = jnp.sum(jnp.where(col == j, work, 0.0), axis=1, keepdims=True)
            line = jnp.sum(jnp.where(row == j, work, 0.0), axis=0, keepdims=True)
            own = jnp.sum(jnp.where(row == j, inverse, 0.0), axis=0, keepdims=True)
            pivot = jnp.max(jnp.where(row[:, :1] == j, column, -jnp.inf), axis=0, keepdims=True)
            ratio = jnp.where(row[:, :1] > j, column / pivot, 0.0)
            w_ref[...] = work - ratio * line
            x_ref[...] = jnp.where(row == j, own / jnp.sqrt(pivot), inverse - ratio * own)
            return carry

        lax.fori_loop(0, RANK, eliminate, 0)

    inverse = jnp.where(row >= col, x_ref[...], 0.0) * scale[...]
    x_ref[...] = inverse
    halves = split(inverse)
    squares = jnp.zeros((1, RANK), f32)
    for q in range(4):
        block = mall[q].reshape(BLOCK, RANK)
        factor = dot_split(split(block), halves) * (1.0 / REPLICAS)
        top, rest = split(factor)
        top_ref[q * BLOCK : (q + 1) * BLOCK] = top
        rest_ref[q * BLOCK : (q + 1) * BLOCK] = rest
        squares = squares + jnp.sum(factor * factor, axis=0, keepdims=True)
    norms = jnp.sqrt(squares + epsilon)
    orthonormal = dot(p_ref[...], inverse, ((1,), (1,)))
    directions = orthonormal / norms * math.sqrt(ROWS * COLS / RANK)

    place = x * 32 + z * 2 + c
    for j in range(4):

        @pl.when(place % 4 == j)
        def _():
            own = mall[place // 32, (place % 32) // 4, OWN * j : OWN * (j + 1)]
            new_f[...] = dot(own, inverse, ((1,), (1,))) * (1.0 / REPLICAS) / norms

    both = split(jnp.concatenate([orthonormal, directions], axis=0))
    width = 256
    copies = []
    for j in range(COLS // width):
        columns = slice(j * width, (j + 1) * width)
        products = dot_split(both, (top_ref[columns, :], rest_ref[columns, :]))
        m_buf[:, columns] = buffer[:, columns] - (1.0 - decay_rate) * products[:SHARD]
        u_buf[:, columns] = products[SHARD:].astype(jnp.bfloat16)
        part = pl.ds(j * width, width)
        copies.append(pltpu.make_async_copy(m_buf.at[:, part], new_m.at[0, :, part], m_sem.at[j]))
        copies.append(pltpu.make_async_copy(u_buf.at[:, part], update.at[:, part], u_sem.at[j]))
        copies[-2].start()
        copies[-1].start()
    for copy in copies:
        copy.wait()


def finish(*gathered):
    vmem = pl.BlockSpec(memory_space=VMEM)
    anywhere = pl.BlockSpec(memory_space=pltpu.HBM)
    return pl.pallas_call(
        finish_kernel,
        name="finish",
        out_shape=(
            jax.ShapeDtypeStruct((1, SHARD, COLS), f32),
            jax.ShapeDtypeStruct((SHARD, COLS), jnp.bfloat16),
            jax.ShapeDtypeStruct((OWN, RANK), f32),
        ),
        in_specs=[vmem] * 7,
        out_specs=(anywhere, anywhere, vmem),
        scratch_shapes=[
            VMEM((RANK, RANK), f32),
            VMEM((RANK, RANK), f32),
            VMEM((COLS, RANK), jnp.bfloat16),
            VMEM((COLS, RANK), jnp.bfloat16),
            VMEM((SHARD, COLS), f32),
            VMEM((SHARD, COLS), jnp.bfloat16),
            pltpu.SemaphoreType.DMA((9,)),
            pltpu.SemaphoreType.DMA((9,)),
        ],
        compiler_params=pltpu.CompilerParams(vmem_limit_bytes=40 * 1024 * 1024),
    )(*gathered)


def shards(momentum, gradient, right_factor):
    return finish(*exchange(momentum, gradient, right_factor))


def solution(mesh):
    split = Mesh(mesh.devices.reshape(mesh.shape["rep"], NX, NZ, 2), ("rep",) + FSDP)
    in_specs = (P("rep", FSDP, None), P("rep", FSDP, None), P(FSDP, None))
    out_specs = (P("rep", FSDP, None), P(FSDP, None), P(FSDP, None))
    return jax.shard_map(
        shards, mesh=split, in_specs=in_specs, out_specs=out_specs, check_vma=False
    )
```

```python
import math

import jax
import jax.numpy as jnp
from jax import lax
from jax.experimental import pallas as pl
from jax.experimental.pallas import tpu as pltpu
from jax.sharding import Mesh
from jax.sharding import PartitionSpec as P

ROWS = 18432
COLS = 2304
RANK = 256
REPLICAS = 4
FSDP = ("fx", "fz", "fc")

NX, NZ = 4, 16
SHARD = ROWS // 128
BLOCK = COLS // 4
PACKED = SHARD * BLOCK // 128
OWN = COLS // 128
PIECE = 80
FACTOR_ROWS = 72
TILES = PIECE // 8

epsilon = 1e-06
decay_rate = 0.95
highest = lax.Precision.HIGHEST
MESH = pl.DeviceIdType.MESH
VMEM = pltpu.VMEM
f32 = jnp.float32


def copy_to(src, dst, send, recv, device):
    return pltpu.make_async_remote_copy(
        src_ref=src,
        dst_ref=dst,
        send_sem=send,
        recv_sem=recv,
        device_id=device,
        device_id_type=MESH,
    )


def took(ref, sem, device):
    copy_to(ref, ref, sem, sem, device).wait_recv()


def gather_ring(block, two, three, me, right, left, send, recv, meanwhile):
    before, after = (me + 3) % 4, (me + 1) % 4

    def hop(q, h, device, i):
        return copy_to(block(q, h), block(q, h), send.at[0], recv.at[i], device)

    first = [hop(me, 0, right, 0), hop(me, 1, left, 1), hop(me, 1, right, 2), hop(me, 0, left, 2)]
    for copy in first:
        copy.start()
    meanwhile()
    first[0].wait_recv()
    hop(before, 0, right, 2).start()
    first[1].wait_recv()
    hop(after, 1, left, 2).start()
    took(two, recv.at[2], right)
    took(three, send.at[0], right)


def split(a):
    top = a.astype(jnp.bfloat16)
    return top, (a - top.astype(f32)).astype(jnp.bfloat16)


ROUGH, FAIR, FULL = 0, 1, 2


def dot(a, b, contract, mode=FULL):
    def product(left, right):
        return lax.dot_general(left, right, (contract, ((), ())), preferred_element_type=f32)

    if mode == FULL:
        return lax.dot_general(a, b, (contract, ((), ())), precision=highest, preferred_element_type=f32)
    if mode == ROUGH:
        return product(a.astype(jnp.bfloat16), b.astype(jnp.bfloat16))
    (a_top, a_rest), (b_top, b_rest) = split(a), split(b)
    return product(a_top, b_top) + (product(a_top, b_rest) + product(a_rest, b_top))


def positions():
    shape = (RANK, RANK)
    return lax.broadcasted_iota(jnp.int32, shape, 0), lax.broadcasted_iota(jnp.int32, shape, 1)


def invert_start(gram, a_ref, x_ref, scale):
    row, col = positions()
    diagonal = jnp.where(row == col, gram, 0.0)
    by_row = lax.rsqrt(jnp.sum(diagonal, axis=1, keepdims=True))
    by_col = lax.rsqrt(jnp.sum(diagonal, axis=0, keepdims=True))
    scaled = gram * by_row * by_col
    a_ref[...] = scaled
    scale[...] = by_col
    bound = jnp.max(jnp.sum(jnp.abs(scaled), axis=0, keepdims=True), axis=1, keepdims=True)
    x_ref[...] = jnp.where(row == col, lax.rsqrt(bound / 2.0), 0.0)


def invert_step(a_ref, x_ref, mode, last=FULL):
    row, col = positions()
    inverse = x_ref[...]
    error = dot(dot(inverse, a_ref[...], ((1,), (0,)), mode), inverse, ((1,), (1,)), mode)
    error = jnp.where(row == col, error - 1.0, error)
    lower = jnp.where(row > col, error, jnp.where(row == col, 0.5 * error, 0.0))
    x_ref[...] = inverse - dot(lower, inverse, ((1,), (0,)), last)
    return error


def exchange_kernel(
    m_hbm, g_hbm, r_hbm, buffer, p_out, mall, a_out, x_out, scale, size,
    mv, gv, rv, bs, raw, comb, cin, inn, packed, s_c, s_t, rall, rc, pall, p_t, mloc, crecv, mx, xrecv, mz, zrecv, fin, zall, gall,
    load, s_send, s_recv, rx_send, rx_recv, rz_send, rz_recv, rc_send, rc_recv, p_send, p_recv,
    c_send, c_recv, x_send, x_recv, z_send, z_recv, f_send, f_recv, a_send, a_recv, b_send, b_recv,
    d_send, d_recv, gx_send, gx_recv, gy_send, gy_recv, gc_send, gc_recv,
):
    y, x, z, c = (lax.axis_index(name) for name in ("rep",) + FSDP)

    def at_y(q):
        return (q, x, z, c)

    def at_x(q):
        return (y, q, z, c)

    def at_z(q):
        return (y, x, q, c)

    partner = (y, x, z, 1 - c)
    peers = [at_z((z + NZ + d) % NZ) for d in (4, -4, 3, -3, 2, -2, 1, -1)]
    peers += [at_y((y + d) % 4) for d in range(1, 4)]
    peers += [at_x((x + d) % 4) for d in range(1, 4)]
    peers += [partner]
    source = x == y
    load_m = pltpu.make_async_copy(m_hbm.at[0], mv, load.at[0])
    load_g = pltpu.make_async_copy(g_hbm.at[0], gv, load.at[1])
    load_r = pltpu.make_async_copy(r_hbm, rv, load.at[2])

    @pl.when(source)
    def _():
        load_r.start()

    load_m.start()
    load_g.start()
    barrier = pltpu.get_barrier_semaphore()
    for peer in peers:
        pl.semaphore_signal(barrier, inc=1, device_id=peer, device_id_type=MESH)

    load_m.wait()
    load_g.wait()
    for q in range(4):
        columns = slice(q * BLOCK, (q + 1) * BLOCK)
        part = mv[:, columns] + gv[:, columns].astype(f32)
        buffer[:, columns] = part
        for t in range(4):
            bs[q, t * SHARD : (t + 1) * SHARD] = part[:, t * 128 : (t + 1) * 128]
        bs[q, 4 * SHARD :, :64] = part[: SHARD // 2, 512:]
        bs[q, 4 * SHARD :, 64:] = part[SHARD // 2 :, 512:]

    @pl.when(source)
    def _():
        load_r.wait()
        rall[z, c, :OWN] = rv[:, :128]
        rall[z, c, OWN:] = rv[:, 128:]

    pl.semaphore_wait(barrier, len(peers))

    to_x = [
        copy_to(rall.at[z, c], rall.at[z, c], rx_send.at[0], rx_recv.at[0], at_x((x + d) % 4))
        for d in range(1, 4)
    ]

    @pl.when(source)
    def _():
        for copy in to_x:
            copy.start()

    half = SHARD // 2
    cut = PACKED // 2 // 8 * 8
    up, down = at_y((y + 1) % 4), at_y((y + 3) % 4)
    after, before, across = (y + 1) % 4, (y + 3) % 4, (y + 2) % 4
    low, high = pl.ds(0, cut), pl.ds(cut, PACKED - cut)
    rest = pl.ds(0, PACKED - cut)
    sums = [
        copy_to(bs.at[across, low], raw.at[0, low], s_send.at[0], s_recv.at[0], up),
        copy_to(bs.at[across, high], raw.at[1, rest], s_send.at[0], s_recv.at[1], down),
        copy_to(bs.at[after, high], inn.at[1, rest], s_send.at[0], s_recv.at[2], up),
        copy_to(bs.at[before, low], inn.at[0, low], s_send.at[0], s_recv.at[2], down),
    ]
    for copy in sums:
        copy.start()

    @pl.when(jnp.logical_not(source))
    def _():
        to_x[0].wait_recv()

    def along_z(owner, far, step):
        block = rall.at[(z + NZ - owner) % NZ, c]
        arrival = {4: 0, -4: 1}.get(far, 2)
        return copy_to(block, block, rz_send.at[0], rz_recv.at[arrival], at_z((z + NZ + step) % NZ))

    to_z = [along_z(0, d, d) for d in (4, -4, 3, -3, 2, -2, 1, -1)]
    for copy in to_z:
        copy.start()

    sums[0].wait_recv()
    comb[0, :cut] = raw[0, :cut] + bs[after, :cut]
    sums.append(copy_to(comb.at[0, low], cin.at[0, low], s_send.at[0], s_recv.at[2], up))
    sums[4].start()
    sums[1].wait_recv()
    comb[1, : PACKED - cut] = raw[1, : PACKED - cut] + bs[before, cut:]
    sums.append(copy_to(comb.at[1, rest], cin.at[1, rest], s_send.at[0], s_recv.at[2], down))
    sums[5].start()

    def hand_along(owner, steps):
        sign = 1 if owner > 0 else -1
        along_z(0, owner, sign).wait_recv()
        for d in steps:
            along_z(owner, owner + sign * d, sign * d).start()

    hand_along(4, (4, 3, 2, 1))
    hand_along(-4, (3, 2, 1))

    took(rall.at[pl.ds(0, 13), c], rz_recv.at[2], partner)
    over = copy_to(rall.at[:, c], rall.at[:, c], rc_send.at[0], rc_recv.at[0], partner)
    over.start()
    took(bs.at[pl.ds(0, 2)], s_recv.at[2], up)
    packed[:cut] = bs[y, :cut] + inn[0, :cut] + cin[0, :cut]
    packed[cut:] = bs[y, cut:] + inn[1, : PACKED - cut] + cin[1, : PACKED - cut]
    for t in range(4):
        s_c[:, t * 128 : (t + 1) * 128] = packed[t * SHARD : (t + 1) * SHARD]
    s_c[: SHARD // 2, 512:] = packed[4 * SHARD :, :64]
    s_c[SHARD // 2 :, 512:] = packed[4 * SHARD :, 64:]
    over.wait_recv()
    for b in range(32):
        rc[b * OWN : (b + 1) * OWN, :128] = rall[b // 2, b % 2, :OWN]
        rc[b * OWN : (b + 1) * OWN, 128:] = rall[b // 2, b % 2, OWN:]
    pall[y] = jnp.dot(s_c[...], rc[...], precision=highest, preferred_element_type=f32)

    def rows_of(q, h):
        return pall.at[q, pl.ds(half * h, half)]

    def turn():
        s_t[...] = s_c[...].T

    gather_ring(
        rows_of, pall.at[pl.ds(0, 2)], pall.at[pl.ds(0, 3)], y, up, down, p_send, p_recv, turn
    )
    projected = pall[0] + pall[1] + pall[2] + pall[3]
    p_out[...] = projected

    p_t[...] = projected.T

    def fill(side):
        wide, narrow = 4 * FACTOR_ROWS, 32
        rows = pl.ds(pl.multiple_of(wide * side, 8), wide)
        gram_rows = pl.ds(pl.multiple_of(2 * narrow * y + narrow * side, 8), narrow)
        left = jnp.concatenate([s_t[rows, :], p_t[gram_rows, :]], axis=0)
        part = jnp.dot(left, projected, precision=highest, preferred_element_type=f32)
        for i in range(4):
            mloc[4 * side + i, :FACTOR_ROWS] = part[i * FACTOR_ROWS : (i + 1) * FACTOR_ROWS]
            mloc[4 * side + i, FACTOR_ROWS:] = part[wide + 8 * i : wide + 8 * i + 8]

    fill(1 - c)
    to_core = copy_to(mloc.at[pl.ds(4 * (1 - c), 4)], crecv, c_send.at[0], c_recv.at[0], partner)
    to_core.start()
    fill(c)
    to_core.wait_recv()
    factor_rows, gram_rows = pl.ds(0, FACTOR_ROWS), pl.ds(FACTOR_ROWS, 8)

    def along_x(d, part, i):
        q = (x + d) % 4
        return copy_to(mx.at[q, part], xrecv.at[d - 1, part], x_send.at[0], x_recv.at[i], at_x(q))

    sums_g = [along_x(d, gram_rows, 0) for d in (2, 1, 3)]
    sums_x = [along_x(d, factor_rows, 1) for d in (2, 1, 3)]
    for q in range(4):
        mx[q] = mloc[4 * c + q] + crecv[q]
    for copy in sums_g + sums_x:
        copy.start()

    owners = [(16 * t + 9) // 10 for t in range(TILES)]
    tile = (z * TILES) // NZ
    owner = (z * TILES) % NZ < TILES
    sums_z = [
        copy_to(mz.at[pl.ds(8 * t, 8)], zrecv.at[z], z_send.at[0], z_recv.at[0], at_z(owners[t]))
        for t in range(TILES)
    ]

    def to_owner(t):
        @pl.when(z != owners[t])
        def _():
            sums_z[t].start()

    took(mz.at[pl.ds(0, 24)], x_recv.at[0], partner)
    mz[FACTOR_ROWS:] = (
        mx[x, FACTOR_ROWS:] + xrecv[0, FACTOR_ROWS:] + xrecv[1, FACTOR_ROWS:] + xrecv[2, FACTOR_ROWS:]
    )
    to_owner(TILES - 1)
    took(mall.at[0, pl.ds(0, 3)], x_recv.at[1], partner)
    mz[:FACTOR_ROWS] = (
        mx[x, :FACTOR_ROWS] + xrecv[0, :FACTOR_ROWS] + xrecv[1, :FACTOR_ROWS] + xrecv[2, :FACTOR_ROWS]
    )
    for t in range(TILES - 1):
        to_owner(t)

    group = 4 * c + x
    rows = pl.ds(pl.multiple_of(8 * tile, 8), 8)
    to_all = [
        copy_to(
            fin, zall.at[rows], f_send.at[0], f_recv.at[tile // (TILES - 1)], at_z((z + d) % NZ)
        )
        for d in sorted(range(1, NZ), key=lambda d: abs(d - NZ // 2))
    ]

    @pl.when(owner)
    def _():
        took(zrecv.at[pl.ds(0, NZ - 1)], z_recv.at[0], partner)
        zrecv[z] = mz[rows, :]
        total = zrecv[0]
        for s in range(1, NZ):
            total = total + zrecv[s]
        fin[...] = total
        for copy in to_all:
            copy.start()
        zall[rows, :] = total

    last = owners[-1]

    @pl.when(z != last)
    def _():
        took(fin, f_recv.at[1], partner)

    gram_x = [
        copy_to(
            zall.at[gram_rows], gall.at[y, group], gx_send.at[0], gx_recv.at[0], at_x((x + d) % 4)
        )
        for d in (2, 1, 3)
    ]
    mine = pl.ds(4 * c, 4)
    gram_y = [
        copy_to(gall.at[y, mine], gall.at[y, mine], gy_send.at[0], gy_recv.at[0], at_y((y + d) % 4))
        for d in (2, 1, 3)
    ]
    gram_core = copy_to(gall.at[:, mine], gall.at[:, mine], gc_send.at[0], gc_recv.at[0], partner)
    for copy in gram_x:
        copy.start()
    gall[y, group] = zall[gram_rows, :]
    took(gall.at[y, pl.ds(0, 3)], gx_recv.at[0], partner)
    for copy in gram_y:
        copy.start()
    owns_factor = owner & (z != last)

    @pl.when(owns_factor)
    def _():
        took(zall.at[pl.ds(0, FACTOR_ROWS - 8)], f_recv.at[0], partner)

    @pl.when(jnp.logical_not(owns_factor))
    def _():
        took(zall.at[pl.ds(0, FACTOR_ROWS)], f_recv.at[0], partner)


    first, second = x * (1 - c) + y * c, y * (1 - c) + x * c

    def turned(a, b):
        return (b * (1 - c) + a * c, a * (1 - c) + b * c)

    def block_of(k, j):
        at, to = turned((first + k) % 4, (second + j) % 4)
        return mall.at[at, 4 * c + to]

    def half_of(k, j, h):
        at, to = turned((first + k) % 4, (second + j) % 4)
        return mall.at[at, 4 * c + to, pl.ds(40 * h, 40 - 8 * h)]

    def source_of(k, j, h):
        return half_of(k, j, h) if k or j else zall.at[pl.ds(40 * h, 40 - 8 * h)]

    def on_first(k, h, step, i):
        device = turned((first + step) % 4, second) + (z, c)
        return copy_to(source_of(k, 0, h), half_of(k, 0, h), a_send.at[0], a_recv.at[i], device)

    def on_second(k, j, h, step, i):
        device = turned(first, (second + step) % 4) + (z, c)
        return copy_to(source_of(k, j, h), half_of(k, j, h), b_send.at[0], b_recv.at[4 * k + (0, 1, 2, 2, 3, 3)[i]], device)

    def on_chip(k, j):
        source = block_of(k, j) if k or j else zall.at[pl.ds(0, FACTOR_ROWS)]
        copy_to(source, block_of(k, j), d_send.at[0], d_recv.at[0], partner).start()

    def half_on_chip(k, j, h):
        copy_to(half_of(k, j, h), half_of(k, j, h), d_send.at[0], d_recv.at[0], partner).start()

    ring = [on_first(0, 0, 1, 0), on_first(0, 1, 3, 1), on_first(0, 1, 1, 2), on_first(0, 0, 3, 3)]
    ring += [on_first(0, 0, 2, 4), on_first(0, 1, 2, 5)]
    across_ring = [
        [on_second(k, 0, 0, 1, 0), on_second(k, 0, 1, 3, 1), on_second(k, 0, 1, 1, 2)]
        + [on_second(k, 0, 0, 3, 3), on_second(k, 3, 0, 1, 4), on_second(k, 1, 1, 3, 5)]
        for k in range(4)
    ]

    def start_half(k, h):
        for i in ((0, 3), (1, 2))[h]:
            across_ring[k][i].start()

    def hand_on(k):
        for i in range(2):
            across_ring[k][i].wait_recv()
            across_ring[k][4 + i].start()
            half_on_chip(k, (3, 1)[i], i)

    def beside(k):
        took(mall.at[0, 0], b_recv.at[4 * k + 2], partner)
        half_on_chip(k, 3, 1)
        half_on_chip(k, 1, 0)

    def complete(k):
        took(mall.at[0, 0], b_recv.at[4 * k + 3], partner)
        on_chip(k, 2)

    for copy in ring[4:] + ring[:4]:
        copy.start()
    start_half(0, 0)
    start_half(0, 1)
    on_chip(0, 0)
    mall[y, group] = zall[:FACTOR_ROWS, :]
    took(gall.at[pl.ds(0, 3), pl.ds(0, 4)], gy_recv.at[0], partner)
    gram_core.start()
    ring[0].wait_recv()
    start_half(3, 0)
    ring[1].wait_recv()
    start_half(1, 1)
    ring[2].wait_recv()
    start_half(3, 1)
    ring[3].wait_recv()
    start_half(1, 0)
    on_chip(3, 0)
    on_chip(1, 0)
    gram_core.wait_recv()
    invert_start(gall[...].reshape(RANK, RANK), a_out, x_out, scale)
    invert_step(a_out, x_out, ROUGH, ROUGH)
    ring[4].wait_recv()
    start_half(2, 0)
    ring[5].wait_recv()
    start_half(2, 1)
    on_chip(2, 0)
    hand_on(0)
    for _ in range(3):
        invert_step(a_out, x_out, ROUGH, ROUGH)
    beside(0)
    hand_on(3)
    hand_on(1)
    for _ in range(2):
        invert_step(a_out, x_out, ROUGH, ROUGH)
    beside(3)
    beside(1)
    hand_on(2)
    complete(0)
    invert_step(a_out, x_out, FAIR, ROUGH)
    beside(2)
    complete(3)
    complete(1)
    complete(2)
    error = invert_step(a_out, x_out, FULL, FAIR)
    size[...] = jnp.sum(jnp.sum(error * error, axis=0, keepdims=True), axis=1, keepdims=True)

    @pl.when(source)
    def _():
        took(rall.at[pl.ds(0, 3), c], rx_send.at[0], partner)

    took(rall.at[pl.ds(0, 15), c], rz_send.at[0], partner)
    took(bs.at[pl.ds(0, 3)], s_send.at[0], partner)
    over.wait_send()
    to_core.wait_send()
    took(mx.at[pl.ds(0, 3)], x_send.at[0], partner)

    @pl.when(owner)
    def _():
        took(zall.at[pl.ds(0, PIECE - 8)], z_send.at[0], partner)
        took(zrecv.at[pl.ds(0, NZ - 1)], f_send.at[0], partner)

    @pl.when(jnp.logical_not(owner))
    def _():
        took(zall, z_send.at[0], partner)

    took(gall.at[y, pl.ds(0, 3)], gx_send.at[0], partner)
    took(gall.at[pl.ds(0, 3), pl.ds(0, 4)], gy_send.at[0], partner)
    gram_core.wait_send()
    took(mall.at[pl.ds(0, 3), 0], a_send.at[0], partner)
    took(mall.at[pl.ds(0, 3), pl.ds(0, 4)], b_send.at[0], partner)
    took(mall.at[:, pl.ds(0, 4)], d_send.at[0], partner)
    took(mall.at[:, pl.ds(0, 4)], d_recv.at[0], partner)


def exchange(momentum, gradient, right_factor):
    sem = pltpu.SemaphoreType.DMA
    longer = PACKED - PACKED // 2 // 8 * 8
    counts = (3, 1, 3, 1, 1, 1, 3, 1, 1, 1, 3, 1, 1, 1, 2, 1, 1, 1, 2, 1, 6, 1, 16) + (1,) * 8
    return pl.pallas_call(
        exchange_kernel,
        name="exchange",
        out_shape=(
            jax.ShapeDtypeStruct((SHARD, COLS), f32),
            jax.ShapeDtypeStruct((SHARD, RANK), f32),
            jax.ShapeDtypeStruct((4, 8, FACTOR_ROWS, RANK), f32),
            jax.ShapeDtypeStruct((RANK, RANK), f32),
            jax.ShapeDtypeStruct((RANK, RANK), f32),
            jax.ShapeDtypeStruct((1, RANK), f32),
            jax.ShapeDtypeStruct((1, 1), f32),
        ),
        in_specs=[pl.BlockSpec(memory_space=pltpu.HBM)] * 3,
        out_specs=(pl.BlockSpec(memory_space=VMEM),) * 7,
        scratch_shapes=[
            VMEM((SHARD, COLS), f32),
            VMEM((SHARD, COLS), jnp.bfloat16),
            VMEM((OWN, RANK), f32),
            VMEM((4, PACKED, 128), f32),
            VMEM((2, longer, 128), f32),
            VMEM((2, longer, 128), f32),
            VMEM((2, longer, 128), f32),
            VMEM((2, longer, 128), f32),
            VMEM((PACKED, 128), f32),
            VMEM((SHARD, BLOCK), f32),
            VMEM((BLOCK, SHARD), f32),
            VMEM((NZ, 2, 2 * OWN, 128), f32),
            VMEM((BLOCK, RANK), f32),
            VMEM((4, SHARD, RANK), f32),
            VMEM((RANK, SHARD), f32),
            VMEM((8, PIECE, RANK), f32),
            VMEM((4, PIECE, RANK), f32),
            VMEM((4, PIECE, RANK), f32),
            VMEM((3, PIECE, RANK), f32),
            VMEM((PIECE, RANK), f32),
            VMEM((NZ, 8, RANK), f32),
            VMEM((8, RANK), f32),
            VMEM((PIECE, RANK), f32),
            VMEM((4, 8, 8, RANK), f32),
        ]
        + [sem((n,)) for n in counts],
        compiler_params=pltpu.CompilerParams(
            collective_id=0, has_side_effects=True, vmem_limit_bytes=40 * 1024 * 1024
        ),
    )(*(pltpu.with_memory_space_constraint(a, pltpu.HBM) for a in (momentum, gradient, right_factor)))


def dot_split(a, b):
    (a_top, a_rest), (b_top, b_rest) = a, b
    turn = (((1,), (1,)), ((), ()))

    def product(left, right):
        return lax.dot_general(left, right, turn, preferred_element_type=f32)

    return product(a_top, b_top) + (product(a_top, b_rest) + product(a_rest, b_top))


def finish_kernel(
    buffer, p_ref, mall, a_ref, x_first, scale, first_size, new_m, update, new_f,
    x_ref, w_ref, top_ref, rest_ref, m_buf, u_buf, m_sem, u_sem,
):
    x, z, c = (lax.axis_index(name) for name in FSDP)

    row, col = positions()
    x_ref[...] = x_first[...]

    def again(state):
        error = invert_step(a_ref, x_ref, FULL)
        return jnp.sum(error * error), state[1] + 1

    size, _ = lax.while_loop(
        lambda s: jnp.logical_not(s[0] <= 3e-5) & (s[1] < 40), again, (jnp.max(first_size[...]), jnp.int32(0))
    )

    @pl.when(jnp.logical_not(size <= 3e-5))
    def _():
        w_ref[...] = a_ref[...]
        x_ref[...] = jnp.where(row == col, 1.0, 0.0)

        def eliminate(j, carry):
            work = w_ref[...]
            inverse = x_ref[...]
            column = jnp.sum(jnp.where(col == j, work, 0.0), axis=1, keepdims=True)
            line = jnp.sum(jnp.where(row == j, work, 0.0), axis=0, keepdims=True)
            own = jnp.sum(jnp.where(row == j, inverse, 0.0), axis=0, keepdims=True)
            pivot = jnp.max(jnp.where(row[:, :1] == j, column, -jnp.inf), axis=0, keepdims=True)
            ratio = jnp.where(row[:, :1] > j, column / pivot, 0.0)
            w_ref[...] = work - ratio * line
            x_ref[...] = jnp.where(row == j, own / jnp.sqrt(pivot), inverse - ratio * own)
            return carry

        lax.fori_loop(0, RANK, eliminate, 0)

    inverse = jnp.where(row >= col, x_ref[...], 0.0) * scale[...]
    x_ref[...] = inverse
    halves = split(inverse * (1.0 / REPLICAS))
    squares = jnp.zeros((1, RANK), f32)
    for q in range(4):
        block = mall[q].reshape(BLOCK, RANK)
        factor = dot_split(split(block), halves)
        top, rest = split(factor)
        top_ref[q * BLOCK : (q + 1) * BLOCK] = top
        rest_ref[q * BLOCK : (q + 1) * BLOCK] = rest
        squares = squares + jnp.sum(factor * factor, axis=0, keepdims=True)
    norms = jnp.sqrt(squares + epsilon)
    orthonormal = dot(p_ref[...], inverse, ((1,), (1,)))
    directions = orthonormal / norms * math.sqrt(ROWS * COLS / RANK)

    place = x * 32 + z * 2 + c
    for j in range(4):

        @pl.when(place % 4 == j)
        def _():
            own = mall[place // 32, (place % 32) // 4, OWN * j : OWN * (j + 1)]
            new_f[...] = dot(own, inverse, ((1,), (1,))) * (1.0 / REPLICAS) / norms

    both = split(jnp.concatenate([orthonormal, directions], axis=0))
    width = 256
    copies = []
    for j in range(COLS // width):
        columns = slice(j * width, (j + 1) * width)
        products = dot_split(both, (top_ref[columns, :], rest_ref[columns, :]))
        m_buf[:, columns] = buffer[:, columns] - (1.0 - decay_rate) * products[:SHARD]
        u_buf[:, columns] = products[SHARD:].astype(jnp.bfloat16)
        part = pl.ds(j * width, width)
        copies.append(pltpu.make_async_copy(m_buf.at[:, part], new_m.at[0, :, part], m_sem.at[j]))
        copies.append(pltpu.make_async_copy(u_buf.at[:, part], update.at[:, part], u_sem.at[j]))
        copies[-2].start()
        copies[-1].start()
    for copy in copies:
        copy.wait()


def finish(*gathered):
    vmem = pl.BlockSpec(memory_space=VMEM)
    anywhere = pl.BlockSpec(memory_space=pltpu.HBM)
    return pl.pallas_call(
        finish_kernel,
        name="finish",
        out_shape=(
            jax.ShapeDtypeStruct((1, SHARD, COLS), f32),
            jax.ShapeDtypeStruct((SHARD, COLS), jnp.bfloat16),
            jax.ShapeDtypeStruct((OWN, RANK), f32),
        ),
        in_specs=[vmem] * 7,
        out_specs=(anywhere, anywhere, vmem),
        scratch_shapes=[
            VMEM((RANK, RANK), f32),
            VMEM((RANK, RANK), f32),
            VMEM((COLS, RANK), jnp.bfloat16),
            VMEM((COLS, RANK), jnp.bfloat16),
            VMEM((SHARD, COLS), f32),
            VMEM((SHARD, COLS), jnp.bfloat16),
            pltpu.SemaphoreType.DMA((9,)),
            pltpu.SemaphoreType.DMA((9,)),
        ],
        compiler_params=pltpu.CompilerParams(vmem_limit_bytes=40 * 1024 * 1024),
    )(*gathered)


def shards(momentum, gradient, right_factor):
    return finish(*exchange(momentum, gradient, right_factor))


def solution(mesh):
    split = Mesh(mesh.devices.reshape(mesh.shape["rep"], NX, NZ, 2), ("rep",) + FSDP)
    in_specs = (P("rep", FSDP, None), P("rep", FSDP, None), P(FSDP, None))
    out_specs = (P("rep", FSDP, None), P(FSDP, None), P(FSDP, None))
    return jax.shard_map(
        shards, mesh=split, in_specs=in_specs, out_specs=out_specs, check_vma=False
    )
```

```python
import math

import jax
import jax.numpy as jnp
from jax import lax
from jax.experimental import pallas as pl
from jax.experimental.pallas import tpu as pltpu
from jax.sharding import Mesh
from jax.sharding import PartitionSpec as P

ROWS = 18432
COLS = 2304
RANK = 256
REPLICAS = 4
FSDP = ("fx", "fz", "fc")

NX, NZ = 4, 16
SHARD = ROWS // 128
BLOCK = COLS // 4
PACKED = SHARD * BLOCK // 128
OWN = COLS // 128
PIECE = 80
FACTOR_ROWS = 72
TILES = PIECE // 8

epsilon = 1e-06
decay_rate = 0.95
highest = lax.Precision.HIGHEST
MESH = pl.DeviceIdType.MESH
VMEM = pltpu.VMEM
f32 = jnp.float32


def copy_to(src, dst, send, recv, device):
    return pltpu.make_async_remote_copy(
        src_ref=src,
        dst_ref=dst,
        send_sem=send,
        recv_sem=recv,
        device_id=device,
        device_id_type=MESH,
    )


def took(ref, sem, device):
    copy_to(ref, ref, sem, sem, device).wait_recv()


def gather_ring(block, two, three, me, right, left, send, recv, meanwhile):
    before, after = (me + 3) % 4, (me + 1) % 4

    def hop(q, h, device, i):
        return copy_to(block(q, h), block(q, h), send.at[0], recv.at[i], device)

    first = [hop(me, 0, right, 0), hop(me, 1, left, 1), hop(me, 1, right, 2), hop(me, 0, left, 2)]
    for copy in first:
        copy.start()
    meanwhile()
    first[0].wait_recv()
    hop(before, 0, right, 2).start()
    first[1].wait_recv()
    hop(after, 1, left, 2).start()
    took(two, recv.at[2], right)
    took(three, send.at[0], right)


def split(a):
    top = a.astype(jnp.bfloat16)
    return top, (a - top.astype(f32)).astype(jnp.bfloat16)


ROUGH, FAIR, FULL = 0, 1, 2


def dot(a, b, contract, mode=FULL):
    def product(left, right):
        return lax.dot_general(left, right, (contract, ((), ())), preferred_element_type=f32)

    if mode == FULL:
        return lax.dot_general(a, b, (contract, ((), ())), precision=highest, preferred_element_type=f32)
    if mode == ROUGH:
        return product(a.astype(jnp.bfloat16), b.astype(jnp.bfloat16))
    (a_top, a_rest), (b_top, b_rest) = split(a), split(b)
    return product(a_top, b_top) + (product(a_top, b_rest) + product(a_rest, b_top))


def positions():
    shape = (RANK, RANK)
    return lax.broadcasted_iota(jnp.int32, shape, 0), lax.broadcasted_iota(jnp.int32, shape, 1)


def invert_start(gram, a_ref, x_ref, scale):
    row, col = positions()
    diagonal = jnp.where(row == col, gram, 0.0)
    by_row = lax.rsqrt(jnp.sum(diagonal, axis=1, keepdims=True))
    by_col = lax.rsqrt(jnp.sum(diagonal, axis=0, keepdims=True))
    scaled = gram * by_row * by_col
    a_ref[...] = scaled
    scale[...] = by_col
    bound = jnp.max(jnp.sum(jnp.abs(scaled), axis=0, keepdims=True), axis=1, keepdims=True)
    x_ref[...] = jnp.where(row == col, lax.rsqrt(bound / 2.0), 0.0)


def invert_step(a_ref, x_ref, mode, last=FULL):
    row, col = positions()
    inverse = x_ref[...]
    error = dot(dot(inverse, a_ref[...], ((1,), (0,)), mode), inverse, ((1,), (1,)), mode)
    error = jnp.where(row == col, error - 1.0, error)
    lower = jnp.where(row > col, error, jnp.where(row == col, 0.5 * error, 0.0))
    x_ref[...] = inverse - dot(lower, inverse, ((1,), (0,)), last)
    return error


def exchange_kernel(
    m_hbm, g_hbm, r_hbm, buffer, p_out, mall, a_out, x_out, scale, size,
    mv, gv, rv, bs, raw, comb, cin, inn, packed, s_c, s_t, rall, rc, pall, p_t, mloc, crecv, mx, xrecv, mz, zrecv, fin, zall, gall,
    load, s_send, s_recv, rx_send, rx_recv, rz_send, rz_recv, rc_send, rc_recv, p_send, p_recv,
    c_send, c_recv, x_send, x_recv, z_send, z_recv, f_send, f_recv, a_send, a_recv, b_send, b_recv,
    d_send, d_recv, gx_send, gx_recv, gy_send, gy_recv, gc_send, gc_recv,
):
    y, x, z, c = (lax.axis_index(name) for name in ("rep",) + FSDP)

    def at_y(q):
        return (q, x, z, c)

    def at_x(q):
        return (y, q, z, c)

    def at_z(q):
        return (y, x, q, c)

    partner = (y, x, z, 1 - c)
    peers = [at_z((z + NZ + d) % NZ) for d in (4, -4, 3, -3, 2, -2, 1, -1)]
    peers += [at_y((y + d) % 4) for d in range(1, 4)]
    peers += [at_x((x + d) % 4) for d in range(1, 4)]
    peers += [partner]
    source = x == y
    cuts = (slice(0, 80), slice(80, SHARD))
    loads = []
    for i, (first, count) in enumerate(((0, 80), (80, SHARD - 80))):
        part = pl.ds(first, count)
        loads.append(
            (
                pltpu.make_async_copy(m_hbm.at[0, part], mv.at[part], load.at[2 * i]),
                pltpu.make_async_copy(g_hbm.at[0, part], gv.at[part], load.at[2 * i + 1]),
            )
        )
    load_r = pltpu.make_async_copy(r_hbm, rv, load.at[4])

    @pl.when(source)
    def _():
        load_r.start()

    for load_m, load_g in loads:
        load_m.start()
        load_g.start()
    barrier = pltpu.get_barrier_semaphore()
    for peer in peers:
        pl.semaphore_signal(barrier, inc=1, device_id=peer, device_id_type=MESH)

    for (load_m, load_g), part in zip(loads, cuts, strict=True):
        load_m.wait()
        load_g.wait()
        for q in range(4):
            columns = slice(q * BLOCK, (q + 1) * BLOCK)
            piece = mv[part, columns] + gv[part, columns].astype(f32)
            buffer[part, columns] = piece
            for t in range(4):
                bs[q, t * SHARD + part.start : t * SHARD + part.stop] = piece[:, t * 128 : (t + 1) * 128]
    for q in range(4):
        columns = slice(q * BLOCK + 512, (q + 1) * BLOCK)
        bs[q, 4 * SHARD :, :64] = buffer[: SHARD // 2, columns]
        bs[q, 4 * SHARD :, 64:] = buffer[SHARD // 2 :, columns]

    @pl.when(source)
    def _():
        load_r.wait()
        rall[z, c, :OWN] = rv[:, :128]
        rall[z, c, OWN:] = rv[:, 128:]

    pl.semaphore_wait(barrier, len(peers))

    to_x = [
        copy_to(rall.at[z, c], rall.at[z, c], rx_send.at[0], rx_recv.at[0], at_x((x + d) % 4))
        for d in range(1, 4)
    ]

    @pl.when(source)
    def _():
        for copy in to_x:
            copy.start()

    half = SHARD // 2
    cut = PACKED // 2 // 8 * 8
    up, down = at_y((y + 1) % 4), at_y((y + 3) % 4)
    after, before, across = (y + 1) % 4, (y + 3) % 4, (y + 2) % 4
    low, high = pl.ds(0, cut), pl.ds(cut, PACKED - cut)
    rest = pl.ds(0, PACKED - cut)
    sums = [
        copy_to(bs.at[across, low], raw.at[0, low], s_send.at[0], s_recv.at[0], up),
        copy_to(bs.at[across, high], raw.at[1, rest], s_send.at[0], s_recv.at[1], down),
        copy_to(bs.at[after, high], inn.at[1, rest], s_send.at[0], s_recv.at[2], up),
        copy_to(bs.at[before, low], inn.at[0, low], s_send.at[0], s_recv.at[2], down),
    ]
    for copy in sums:
        copy.start()

    @pl.when(jnp.logical_not(source))
    def _():
        to_x[0].wait_recv()

    def along_z(owner, far, step):
        block = rall.at[(z + NZ - owner) % NZ, c]
        arrival = {4: 0, -4: 1}.get(far, 2)
        return copy_to(block, block, rz_send.at[0], rz_recv.at[arrival], at_z((z + NZ + step) % NZ))

    to_z = [along_z(0, d, d) for d in (4, -4, 3, -3, 2, -2, 1, -1)]
    for copy in to_z:
        copy.start()

    sums[0].wait_recv()
    comb[0, :cut] = raw[0, :cut] + bs[after, :cut]
    sums.append(copy_to(comb.at[0, low], cin.at[0, low], s_send.at[0], s_recv.at[2], up))
    sums[4].start()
    sums[1].wait_recv()
    comb[1, : PACKED - cut] = raw[1, : PACKED - cut] + bs[before, cut:]
    sums.append(copy_to(comb.at[1, rest], cin.at[1, rest], s_send.at[0], s_recv.at[2], down))
    sums[5].start()

    def hand_along(owner, steps):
        sign = 1 if owner > 0 else -1
        along_z(0, owner, sign).wait_recv()
        for d in steps:
            along_z(owner, owner + sign * d, sign * d).start()

    hand_along(4, (4, 3, 2, 1))
    hand_along(-4, (3, 2, 1))

    took(rall.at[pl.ds(0, 13), c], rz_recv.at[2], partner)
    over = copy_to(rall.at[:, c], rall.at[:, c], rc_send.at[0], rc_recv.at[0], partner)
    over.start()
    took(bs.at[pl.ds(0, 2)], s_recv.at[2], up)
    packed[:cut] = bs[y, :cut] + inn[0, :cut] + cin[0, :cut]
    packed[cut:] = bs[y, cut:] + inn[1, : PACKED - cut] + cin[1, : PACKED - cut]
    for t in range(4):
        s_c[:, t * 128 : (t + 1) * 128] = packed[t * SHARD : (t + 1) * SHARD]
    s_c[: SHARD // 2, 512:] = packed[4 * SHARD :, :64]
    s_c[SHARD // 2 :, 512:] = packed[4 * SHARD :, 64:]
    over.wait_recv()
    for b in range(32):
        rc[b * OWN : (b + 1) * OWN, :128] = rall[b // 2, b % 2, :OWN]
        rc[b * OWN : (b + 1) * OWN, 128:] = rall[b // 2, b % 2, OWN:]
    pall[y] = jnp.dot(s_c[...], rc[...], precision=highest, preferred_element_type=f32)

    def rows_of(q, h):
        return pall.at[q, pl.ds(half * h, half)]

    def turn():
        s_t[...] = s_c[...].T

    gather_ring(
        rows_of, pall.at[pl.ds(0, 2)], pall.at[pl.ds(0, 3)], y, up, down, p_send, p_recv, turn
    )
    projected = pall[0] + pall[1] + pall[2] + pall[3]
    p_out[...] = projected

    p_t[...] = projected.T

    def fill(side):
        wide, narrow = 4 * FACTOR_ROWS, 32
        rows = pl.ds(pl.multiple_of(wide * side, 8), wide)
        gram_rows = pl.ds(pl.multiple_of(2 * narrow * y + narrow * side, 8), narrow)
        left = jnp.concatenate([s_t[rows, :], p_t[gram_rows, :]], axis=0)
        part = jnp.dot(left, projected, precision=highest, preferred_element_type=f32)
        for i in range(4):
            mloc[4 * side + i, :FACTOR_ROWS] = part[i * FACTOR_ROWS : (i + 1) * FACTOR_ROWS]
            mloc[4 * side + i, FACTOR_ROWS:] = part[wide + 8 * i : wide + 8 * i + 8]

    fill(1 - c)
    to_core = copy_to(mloc.at[pl.ds(4 * (1 - c), 4)], crecv, c_send.at[0], c_recv.at[0], partner)
    to_core.start()
    fill(c)
    to_core.wait_recv()
    factor_rows, gram_rows = pl.ds(0, FACTOR_ROWS), pl.ds(FACTOR_ROWS, 8)

    def along_x(d, part, i):
        q = (x + d) % 4
        return copy_to(mx.at[q, part], xrecv.at[d - 1, part], x_send.at[0], x_recv.at[i], at_x(q))

    sums_g = [along_x(d, gram_rows, 0) for d in (2, 1, 3)]
    sums_x = [along_x(d, factor_rows, 1) for d in (2, 1, 3)]
    for q in range(4):
        mx[q] = mloc[4 * c + q] + crecv[q]
    for copy in sums_g + sums_x:
        copy.start()

    owners = [(16 * t + 9) // 10 for t in range(TILES)]
    tile = (z * TILES) // NZ
    owner = (z * TILES) % NZ < TILES
    sums_z = [
        copy_to(mz.at[pl.ds(8 * t, 8)], zrecv.at[z], z_send.at[0], z_recv.at[0], at_z(owners[t]))
        for t in range(TILES)
    ]

    def to_owner(t):
        @pl.when(z != owners[t])
        def _():
            sums_z[t].start()

    took(mz.at[pl.ds(0, 24)], x_recv.at[0], partner)
    mz[FACTOR_ROWS:] = (
        mx[x, FACTOR_ROWS:] + xrecv[0, FACTOR_ROWS:] + xrecv[1, FACTOR_ROWS:] + xrecv[2, FACTOR_ROWS:]
    )
    to_owner(TILES - 1)
    took(mall.at[0, pl.ds(0, 3)], x_recv.at[1], partner)
    mz[:FACTOR_ROWS] = (
        mx[x, :FACTOR_ROWS] + xrecv[0, :FACTOR_ROWS] + xrecv[1, :FACTOR_ROWS] + xrecv[2, :FACTOR_ROWS]
    )
    for t in range(TILES - 1):
        to_owner(t)

    group = 4 * c + x
    rows = pl.ds(pl.multiple_of(8 * tile, 8), 8)
    to_all = [
        copy_to(
            fin, zall.at[rows], f_send.at[0], f_recv.at[tile // (TILES - 1)], at_z((z + d) % NZ)
        )
        for d in sorted(range(1, NZ), key=lambda d: abs(d - NZ // 2))
    ]

    @pl.when(owner)
    def _():
        took(zrecv.at[pl.ds(0, NZ - 1)], z_recv.at[0], partner)
        zrecv[z] = mz[rows, :]
        total = zrecv[0]
        for s in range(1, NZ):
            total = total + zrecv[s]
        fin[...] = total
        for copy in to_all:
            copy.start()
        zall[rows, :] = total

    last = owners[-1]

    @pl.when(z != last)
    def _():
        took(fin, f_recv.at[1], partner)

    gram_x = [
        copy_to(
            zall.at[gram_rows], gall.at[y, group], gx_send.at[0], gx_recv.at[0], at_x((x + d) % 4)
        )
        for d in (2, 1, 3)
    ]
    mine = pl.ds(4 * c, 4)
    gram_y = [
        copy_to(gall.at[y, mine], gall.at[y, mine], gy_send.at[0], gy_recv.at[0], at_y((y + d) % 4))
        for d in (2, 1, 3)
    ]
    gram_core = copy_to(gall.at[:, mine], gall.at[:, mine], gc_send.at[0], gc_recv.at[0], partner)
    for copy in gram_x:
        copy.start()
    gall[y, group] = zall[gram_rows, :]
    took(gall.at[y, pl.ds(0, 3)], gx_recv.at[0], partner)
    for copy in gram_y:
        copy.start()
    owns_factor = owner & (z != last)

    @pl.when(owns_factor)
    def _():
        took(zall.at[pl.ds(0, FACTOR_ROWS - 8)], f_recv.at[0], partner)

    @pl.when(jnp.logical_not(owns_factor))
    def _():
        took(zall.at[pl.ds(0, FACTOR_ROWS)], f_recv.at[0], partner)


    first, second = x * (1 - c) + y * c, y * (1 - c) + x * c

    def turned(a, b):
        return (b * (1 - c) + a * c, a * (1 - c) + b * c)

    def block_of(k, j):
        at, to = turned((first + k) % 4, (second + j) % 4)
        return mall.at[at, 4 * c + to]

    def half_of(k, j, h):
        at, to = turned((first + k) % 4, (second + j) % 4)
        return mall.at[at, 4 * c + to, pl.ds(40 * h, 40 - 8 * h)]

    def source_of(k, j, h):
        return half_of(k, j, h) if k or j else zall.at[pl.ds(40 * h, 40 - 8 * h)]

    def on_first(k, h, step, i):
        device = turned((first + step) % 4, second) + (z, c)
        return copy_to(source_of(k, 0, h), half_of(k, 0, h), a_send.at[0], a_recv.at[i], device)

    def on_second(k, j, h, step, i):
        device = turned(first, (second + step) % 4) + (z, c)
        return copy_to(source_of(k, j, h), half_of(k, j, h), b_send.at[0], b_recv.at[4 * k + (0, 1, 2, 2, 3, 3)[i]], device)

    def on_chip(k, j):
        source = block_of(k, j) if k or j else zall.at[pl.ds(0, FACTOR_ROWS)]
        copy_to(source, block_of(k, j), d_send.at[0], d_recv.at[0], partner).start()

    def half_on_chip(k, j, h):
        copy_to(half_of(k, j, h), half_of(k, j, h), d_send.at[0], d_recv.at[0], partner).start()

    ring = [on_first(0, 0, 1, 0), on_first(0, 1, 3, 1), on_first(0, 1, 1, 2), on_first(0, 0, 3, 3)]
    ring += [on_first(0, 0, 2, 4), on_first(0, 1, 2, 5)]
    across_ring = [
        [on_second(k, 0, 0, 1, 0), on_second(k, 0, 1, 3, 1), on_second(k, 0, 1, 1, 2)]
        + [on_second(k, 0, 0, 3, 3), on_second(k, 3, 0, 1, 4), on_second(k, 1, 1, 3, 5)]
        for k in range(4)
    ]

    def start_half(k, h):
        for i in ((0, 3), (1, 2))[h]:
            across_ring[k][i].start()

    def hand_on(k):
        for i in range(2):
            across_ring[k][i].wait_recv()
            across_ring[k][4 + i].start()
            half_on_chip(k, (3, 1)[i], i)

    def beside(k):
        took(mall.at[0, 0], b_recv.at[4 * k + 2], partner)
        half_on_chip(k, 3, 1)
        half_on_chip(k, 1, 0)

    def complete(k):
        took(mall.at[0, 0], b_recv.at[4 * k + 3], partner)
        on_chip(k, 2)

    for copy in ring[4:] + ring[:4]:
        copy.start()
    start_half(0, 0)
    start_half(0, 1)
    on_chip(0, 0)
    mall[y, group] = zall[:FACTOR_ROWS, :]
    took(gall.at[pl.ds(0, 3), pl.ds(0, 4)], gy_recv.at[0], partner)
    gram_core.start()
    ring[0].wait_recv()
    start_half(3, 0)
    ring[1].wait_recv()
    start_half(1, 1)
    ring[2].wait_recv()
    start_half(3, 1)
    ring[3].wait_recv()
    start_half(1, 0)
    on_chip(3, 0)
    on_chip(1, 0)
    gram_core.wait_recv()
    invert_start(gall[...].reshape(RANK, RANK), a_out, x_out, scale)
    invert_step(a_out, x_out, ROUGH, ROUGH)
    ring[4].wait_recv()
    start_half(2, 0)
    ring[5].wait_recv()
    start_half(2, 1)
    on_chip(2, 0)
    hand_on(0)
    for _ in range(3):
        invert_step(a_out, x_out, ROUGH, ROUGH)
    beside(0)
    hand_on(3)
    hand_on(1)
    for _ in range(2):
        invert_step(a_out, x_out, ROUGH, ROUGH)
    beside(3)
    beside(1)
    hand_on(2)
    complete(0)
    invert_step(a_out, x_out, FAIR, ROUGH)
    beside(2)
    complete(3)
    complete(1)
    complete(2)
    error = invert_step(a_out, x_out, FULL, FAIR)
    size[...] = jnp.sum(jnp.sum(error * error, axis=0, keepdims=True), axis=1, keepdims=True)

    @pl.when(source)
    def _():
        took(rall.at[pl.ds(0, 3), c], rx_send.at[0], partner)

    took(rall.at[pl.ds(0, 15), c], rz_send.at[0], partner)
    took(bs.at[pl.ds(0, 3)], s_send.at[0], partner)
    over.wait_send()
    to_core.wait_send()
    took(mx.at[pl.ds(0, 3)], x_send.at[0], partner)

    @pl.when(owner)
    def _():
        took(zall.at[pl.ds(0, PIECE - 8)], z_send.at[0], partner)
        took(zrecv.at[pl.ds(0, NZ - 1)], f_send.at[0], partner)

    @pl.when(jnp.logical_not(owner))
    def _():
        took(zall, z_send.at[0], partner)

    took(gall.at[y, pl.ds(0, 3)], gx_send.at[0], partner)
    took(gall.at[pl.ds(0, 3), pl.ds(0, 4)], gy_send.at[0], partner)
    gram_core.wait_send()
    took(mall.at[pl.ds(0, 3), 0], a_send.at[0], partner)
    took(mall.at[pl.ds(0, 3), pl.ds(0, 4)], b_send.at[0], partner)
    took(mall.at[:, pl.ds(0, 4)], d_send.at[0], partner)
    took(mall.at[:, pl.ds(0, 4)], d_recv.at[0], partner)


def exchange(momentum, gradient, right_factor):
    sem = pltpu.SemaphoreType.DMA
    longer = PACKED - PACKED // 2 // 8 * 8
    counts = (5, 1, 3, 1, 1, 1, 3, 1, 1, 1, 3, 1, 1, 1, 2, 1, 1, 1, 2, 1, 6, 1, 16) + (1,) * 8
    return pl.pallas_call(
        exchange_kernel,
        name="exchange",
        out_shape=(
            jax.ShapeDtypeStruct((SHARD, COLS), f32),
            jax.ShapeDtypeStruct((SHARD, RANK), f32),
            jax.ShapeDtypeStruct((4, 8, FACTOR_ROWS, RANK), f32),
            jax.ShapeDtypeStruct((RANK, RANK), f32),
            jax.ShapeDtypeStruct((RANK, RANK), f32),
            jax.ShapeDtypeStruct((1, RANK), f32),
            jax.ShapeDtypeStruct((1, 1), f32),
        ),
        in_specs=[pl.BlockSpec(memory_space=pltpu.HBM)] * 3,
        out_specs=(pl.BlockSpec(memory_space=VMEM),) * 7,
        scratch_shapes=[
            VMEM((SHARD, COLS), f32),
            VMEM((SHARD, COLS), jnp.bfloat16),
            VMEM((OWN, RANK), f32),
            VMEM((4, PACKED, 128), f32),
            VMEM((2, longer, 128), f32),
            VMEM((2, longer, 128), f32),
            VMEM((2, longer, 128), f32),
            VMEM((2, longer, 128), f32),
            VMEM((PACKED, 128), f32),
            VMEM((SHARD, BLOCK), f32),
            VMEM((BLOCK, SHARD), f32),
            VMEM((NZ, 2, 2 * OWN, 128), f32),
            VMEM((BLOCK, RANK), f32),
            VMEM((4, SHARD, RANK), f32),
            VMEM((RANK, SHARD), f32),
            VMEM((8, PIECE, RANK), f32),
            VMEM((4, PIECE, RANK), f32),
            VMEM((4, PIECE, RANK), f32),
            VMEM((3, PIECE, RANK), f32),
            VMEM((PIECE, RANK), f32),
            VMEM((NZ, 8, RANK), f32),
            VMEM((8, RANK), f32),
            VMEM((PIECE, RANK), f32),
            VMEM((4, 8, 8, RANK), f32),
        ]
        + [sem((n,)) for n in counts],
        compiler_params=pltpu.CompilerParams(
            collective_id=0, has_side_effects=True, vmem_limit_bytes=40 * 1024 * 1024
        ),
    )(*(pltpu.with_memory_space_constraint(a, pltpu.HBM) for a in (momentum, gradient, right_factor)))


def dot_split(a, b):
    (a_top, a_rest), (b_top, b_rest) = a, b
    turn = (((1,), (1,)), ((), ()))

    def product(left, right):
        return lax.dot_general(left, right, turn, preferred_element_type=f32)

    return product(a_top, b_top) + (product(a_top, b_rest) + product(a_rest, b_top))


def finish_kernel(
    buffer, p_ref, mall, a_ref, x_first, scale, first_size, new_m, update, new_f,
    x_ref, w_ref, own_ref, top_ref, rest_ref, m_buf, u_buf, m_sem, u_sem,
):
    x, z, c = (lax.axis_index(name) for name in FSDP)

    row, col = positions()
    x_ref[...] = x_first[...]
    own_ref[...] = jnp.zeros_like(own_ref)

    def again(state):
        error = invert_step(a_ref, x_ref, FULL)
        return jnp.sum(error * error), state[1] + 1

    size, _ = lax.while_loop(
        lambda s: jnp.logical_not(s[0] <= 3e-5) & (s[1] < 40), again, (jnp.max(first_size[...]), jnp.int32(0))
    )

    @pl.when(jnp.logical_not(size <= 3e-5))
    def _():
        w_ref[...] = a_ref[...]
        x_ref[...] = jnp.where(row == col, 1.0, 0.0)

        def eliminate(j, carry):
            work = w_ref[...]
            inverse = x_ref[...]
            column = jnp.sum(jnp.where(col == j, work, 0.0), axis=1, keepdims=True)
            line = jnp.sum(jnp.where(row == j, work, 0.0), axis=0, keepdims=True)
            own = jnp.sum(jnp.where(row == j, inverse, 0.0), axis=0, keepdims=True)
            pivot = jnp.max(jnp.where(row[:, :1] == j, column, -jnp.inf), axis=0, keepdims=True)
            ratio = jnp.where(row[:, :1] > j, column / pivot, 0.0)
            w_ref[...] = work - ratio * line
            x_ref[...] = jnp.where(row == j, own / jnp.sqrt(pivot), inverse - ratio * own)
            return carry

        lax.fori_loop(0, RANK, eliminate, 0)

    inverse = jnp.where(row >= col, x_ref[...], 0.0) * scale[...]
    x_ref[...] = inverse
    halves = split(inverse * (1.0 / REPLICAS))
    squares = jnp.zeros((1, RANK), f32)
    for q in range(4):
        block = mall[q].reshape(BLOCK, RANK)
        factor = dot_split(split(block), halves)
        top, rest = split(factor)
        top_ref[q * BLOCK : (q + 1) * BLOCK] = top
        rest_ref[q * BLOCK : (q + 1) * BLOCK] = rest
        squares = squares + jnp.sum(factor * factor, axis=0, keepdims=True)
    norms = jnp.sqrt(squares + epsilon)
    place = x * 32 + z * 2 + c
    for j in range(4):

        @pl.when(place % 4 == j)
        def _():
            own_ref[:OWN] = mall[place // 32, (place % 32) // 4, OWN * j : OWN * (j + 1)]

    solved = dot(jnp.concatenate([p_ref[...], own_ref[...]], axis=0), inverse, ((1,), (1,)))
    orthonormal = solved[:SHARD]
    new_f[...] = solved[SHARD : SHARD + OWN] * (1.0 / REPLICAS) / norms
    directions = orthonormal / norms * math.sqrt(ROWS * COLS / RANK)

    both = split(jnp.concatenate([orthonormal, directions], axis=0))
    width = 256
    copies = []
    for j in range(COLS // width):
        columns = slice(j * width, (j + 1) * width)
        products = dot_split(both, (top_ref[columns, :], rest_ref[columns, :]))
        m_buf[:, columns] = buffer[:, columns] - (1.0 - decay_rate) * products[:SHARD]
        u_buf[:, columns] = products[SHARD:].astype(jnp.bfloat16)
        part = pl.ds(j * width, width)
        copies.append(pltpu.make_async_copy(m_buf.at[:, part], new_m.at[0, :, part], m_sem.at[j]))
        copies.append(pltpu.make_async_copy(u_buf.at[:, part], update.at[:, part], u_sem.at[j]))
        copies[-2].start()
        copies[-1].start()
    for copy in copies:
        copy.wait()


def finish(*gathered):
    vmem = pl.BlockSpec(memory_space=VMEM)
    anywhere = pl.BlockSpec(memory_space=pltpu.HBM)
    return pl.pallas_call(
        finish_kernel,
        name="finish",
        out_shape=(
            jax.ShapeDtypeStruct((1, SHARD, COLS), f32),
            jax.ShapeDtypeStruct((SHARD, COLS), jnp.bfloat16),
            jax.ShapeDtypeStruct((OWN, RANK), f32),
        ),
        in_specs=[vmem] * 7,
        out_specs=(anywhere, anywhere, vmem),
        scratch_shapes=[
            VMEM((RANK, RANK), f32),
            VMEM((RANK, RANK), f32),
            VMEM((24, RANK), f32),
            VMEM((COLS, RANK), jnp.bfloat16),
            VMEM((COLS, RANK), jnp.bfloat16),
            VMEM((SHARD, COLS), f32),
            VMEM((SHARD, COLS), jnp.bfloat16),
            pltpu.SemaphoreType.DMA((9,)),
            pltpu.SemaphoreType.DMA((9,)),
        ],
        compiler_params=pltpu.CompilerParams(vmem_limit_bytes=40 * 1024 * 1024),
    )(*gathered)


def shards(momentum, gradient, right_factor):
    return finish(*exchange(momentum, gradient, right_factor))


def solution(mesh):
    split = Mesh(mesh.devices.reshape(mesh.shape["rep"], NX, NZ, 2), ("rep",) + FSDP)
    in_specs = (P("rep", FSDP, None), P("rep", FSDP, None), P(FSDP, None))
    out_specs = (P("rep", FSDP, None), P(FSDP, None), P(FSDP, None))
    return jax.shard_map(
        shards, mesh=split, in_specs=in_specs, out_specs=out_specs, check_vma=False
    )
```
